32 devices in a mesh: parts: 2 (over y), gz: 4 (over z), gy: 2 (over x), lc: 2 (over core).
Axes of the slice: x: 2, y: 2, z: 4, core: 2. Of those that a mesh axis runs over, the one named last changes fastest.
Arguments:
- density: float32 [64, 128, 256], P(('parts', 'gz'), 'gy'), parts along dimension 0, may hold values from 0.05 to 1
- void_mask: int32 [64, 128, 256], P(('parts', 'gz'), 'gy'), parts along dimension 0, may hold values 0 or 1
- fixed_mask: int32 [64, 128, 256], P(('parts', 'gz'), 'gy'), parts along dimension 0, may hold values 0 or 1
- displacement: float32 [2, 3, 64, 128, 256], P('lc', None, ('parts', 'gz'), 'gy'), parts along dimension 2, may hold values from -4 to 4
- load_ratio: int32 [4], P('parts'), parts along dimension 0, may hold values from 1 to 8
Outputs:
- gradient: float32 [64, 128, 256], P(('parts', 'gz'), 'gy'), parts along dimension 0
The draws below stay inside these ranges and needn't reach their ends.
There are 2 independent parts, one for each index of `parts`. The reference program is written for one: setup_inputs(seed, part) draws one part's arguments, and reference() takes and returns one part's arrays. A program takes and returns all parts, laid end to end along the dimension named above; each array names one. Nothing has to cross between parts.
All inputs are finite; a program needn't handle non-finite values. No bound on the sum of `void_mask` or of `fixed_mask` on one device may be relied on, other than what follows from the above.
Results may differ from the reference program's by a relative error of at most 0.0001.
Values sent between devices are 32-bit elements; how exact they have to be, the bound alone decides.
A program may use at most 64 MiB of HBM per device.

```python
import math
import jax
import jax.numpy as jnp
import numpy as np
from jax import lax

NZ = 256
NX = 32
NY = 128
LC = 2


def with_ends(values, rng, low, high):
    dims = values.shape
    spot = [jax.random.randint(jax.random.fold_in(rng, axis), (), 0, dims[axis]) for axis in range(len(dims))]
    values = values.at[tuple(spot)].set(low)
    longest = dims.index(max(dims))
    spot[longest] = (spot[longest] + 1) % dims[longest]
    return values.at[tuple(spot)].set(high)


def block_scale(key, extent, cuts, least, top_value):
    factor_of, own = 1.0, jax.random.fold_in(key, 6)
    for axis_at, shards_of in cuts:
        steps = jnp.exp(jax.random.uniform(jax.random.fold_in(own, axis_at), (shards_of,), jnp.float32, least / len(cuts), top_value / len(cuts)))
        factor_of = factor_of * jnp.repeat(steps, extent[axis_at] // shards_of).reshape([-1 if axis == axis_at else 1 for axis in range(len(extent))])
    return factor_of


def scatter_about(own_key, dims, deviation, bound, cuts=(), kind=jnp.bfloat16):
    gain = block_scale(own_key, dims, cuts, -0.22, 0.18) if cuts else 1.0
    entries = jax.random.normal(own_key, dims, jnp.float32) * deviation * gain
    return jnp.minimum(jnp.maximum(entries, -bound), bound).astype(kind)


def setup_inputs(seed: int = 0, part: int = 0) -> dict:
    key_list = jax.random.split(jax.random.key(seed), 6)
    part_keys = jax.random.split(jax.random.fold_in(key_list[5], part), 6)
    return {
        "density": jnp.clip(0.05 + 0.95 * jax.random.uniform(part_keys[0], (NX, NY, NZ), jnp.float32) ** block_scale(part_keys[0], (NX, NY, NZ), ((0, 4), (1, 2)), -0.2, 0.2), 0.05, 1.0),
        "void_mask": with_ends((jax.random.randint(part_keys[1], (NX, NY, NZ), 0, 8) < 1).astype(jnp.int32), jax.random.fold_in(part_keys[1], 1), 0, 1),
        "fixed_mask": with_ends((jax.random.randint(part_keys[2], (NX, NY, NZ), 0, 8) < 1).astype(jnp.int32), jax.random.fold_in(part_keys[2], 1), 0, 1),
        "displacement": scatter_about(part_keys[3], (LC, 3, NX, NY, NZ), 0.3, 4.0, ((0, 2), (2, 4), (3, 2)), jnp.float32),
        "load_ratio": jax.random.randint(part_keys[4], (LC,), 1, 9).astype(jnp.int32),
    }


def element_stiffness():
    poisson = 0.3
    factor = 1.0 / ((1.0 + poisson) * (1.0 - 2.0 * poisson))
    material = np.zeros((6, 6))
    material[:3, :3] = poisson
    for index in range(3):
        material[index, index] = 1.0 - poisson
        material[index + 3, index + 3] = 0.5 - poisson
    material = material * factor
    corners = [(first, second, third) for first in (0, 1) for second in (0, 1) for third in (0, 1)]
    points = [0.5 - 0.5 / math.sqrt(3.0), 0.5 + 0.5 / math.sqrt(3.0)]
    stiffness = np.zeros((24, 24))
    for point_x in points:
        for point_y in points:
            for point_z in points:
                strain = np.zeros((6, 24))
                for corner_index, (first, second, third) in enumerate(corners):
                    along_x = point_x if first else 1.0 - point_x
                    along_y = point_y if second else 1.0 - point_y
                    along_z = point_z if third else 1.0 - point_z
                    sign_x = 1.0 if first else -1.0
                    sign_y = 1.0 if second else -1.0
                    sign_z = 1.0 if third else -1.0
                    deriv_x = sign_x * along_y * along_z
                    deriv_y = along_x * sign_y * along_z
                    deriv_z = along_x * along_y * sign_z
                    column = 3 * corner_index
                    strain[0, column] = deriv_x
                    strain[1, column + 1] = deriv_y
                    strain[2, column + 2] = deriv_z
                    strain[3, column] = deriv_y
                    strain[3, column + 1] = deriv_x
                    strain[4, column + 1] = deriv_z
                    strain[4, column + 2] = deriv_y
                    strain[5, column] = deriv_z
                    strain[5, column + 2] = deriv_x
                stiffness = stiffness + 0.125 * strain.T @ material @ strain
    return stiffness

def cone_offsets():
    result = []
    for shift_x in range(-2, 3):
        for shift_y in range(-2, 3):
            for shift_z in range(-2, 3):
                dist_sq = shift_x * shift_x + shift_y * shift_y + shift_z * shift_z
                if dist_sq < 6.25:
                    result.append((shift_x, shift_y, shift_z, 2.5 - math.sqrt(dist_sq)))
    return result

def cone_filter(padded, shape):
    rows_x, rows_y, depth = shape
    total = jnp.zeros(shape, padded.dtype)
    for shift_x, shift_y, shift_z, weight in cone_offsets():
        total = total + weight * padded[2 + shift_x:2 + shift_x + rows_x, 2 + shift_y:2 + shift_y + rows_y, 2 + shift_z:2 + shift_z + depth]
    return total

def strain_energy(moved):
    rows_x, rows_y, depth = (moved.shape[1], moved.shape[2], moved.shape[3])
    extended = jnp.pad(moved, ((0, 0), (0, 1), (0, 1), (0, 1)))
    stiffness = jnp.asarray(element_stiffness(), moved.dtype)

    def one_layer(layer):
        layers = lax.dynamic_slice_in_dim(extended, layer, 2, 1)
        nodes = []
        for first in (0, 1):
            for second in (0, 1):
                for third in (0, 1):
                    nodes.append(layers[:, first, second:second + rows_y, third:third + depth])
        flat = jnp.stack(nodes, 0).reshape(24, rows_y * depth)
        product = jnp.dot(stiffness, flat, precision=lax.Precision.HIGHEST)
        return lax.optimization_barrier(jnp.sum(flat * product, 0)).reshape(rows_y, depth)
    return lax.map(one_layer, jnp.arange(rows_x, dtype=jnp.int32))

def reference(density, void_mask, fixed_mask, displacement, load_ratio):
    shape = density.shape
    weight_sum = cone_filter(jnp.pad(jnp.ones_like(density), 2), shape)
    physical = cone_filter(jnp.pad(density, 2), shape) / weight_sum
    free = (1 - fixed_mask).astype(density.dtype)
    ratios = load_ratio.astype(density.dtype)
    shares = ratios / jnp.sum(ratios)
    weighted = jnp.zeros(shape, density.dtype)
    for case in range(displacement.shape[0]):
        energy = strain_energy(displacement[case] * free[None])
        weighted = weighted + shares[case] * energy
    alive = (1 - void_mask).astype(density.dtype)
    sensed = alive * (-3.0 * physical * physical * (1.0 - 0.001)) * weighted / weight_sum
    return alive * cone_filter(jnp.pad(sensed, 2), shape)
```

```python
import math

import jax
import jax.numpy as jnp
from jax import lax
from jax.experimental import pallas as pl
from jax.experimental.pallas import tpu as pltpu
from jax.sharding import PartitionSpec as P

MESH = pl.DeviceIdType.MESH
POISSON = 0.3
FACTOR = 1.0 / ((1.0 + POISSON) * (1.0 - 2.0 * POISSON))
LAMBDA = POISSON * FACTOR
SHEAR = (0.5 - POISSON) * FACTOR
W = [2.5 - math.sqrt(d) for d in range(7)]
N_COPIES = 32
TALL = 32
SHORT = 8


def layer_classes(q0, q1, q2, q4, q5):
    p0 = W[0] * q0 + W[1] * q1 + W[2] * q2 + W[4] * q4 + W[5] * q5
    p1 = W[1] * q0 + W[2] * q1 + W[3] * q2 + W[5] * q4 + W[6] * q5
    p2 = W[4] * q0 + W[5] * q1 + W[6] * q2
    return p0, p1, p2


def lane_index(shape):
    return lax.broadcasted_iota(jnp.int32, shape, len(shape) - 1)


def lane_pair(field, step):
    depth = field.shape[-1]
    lane = lane_index(field.shape)
    after = jnp.where(lane < depth - step, pltpu.roll(field, depth - step, 1), 0.0)
    before = jnp.where(lane >= step, pltpu.roll(field, step, 1), 0.0)
    return after + before


def cone_tiles(ref, layer, row, count):
    window = TALL + 16
    f = [ref[layer + k, pl.ds(row, window), :] for k in range(count + 4)]
    mid = slice(8, 8 + TALL)

    def pair(t, step):
        return (pltpu.roll(t, step, 0) + pltpu.roll(t, window - step, 0))[mid]

    result = []
    for k in range(count):
        x0, x1, x2 = f[k + 2], f[k + 1] + f[k + 3], f[k] + f[k + 4]
        q0 = x0[mid]
        q1 = x1[mid] + pair(x0, 1)
        q2 = pair(x1, 1)
        q4 = x2[mid] + pair(x0, 2)
        q5 = pair(x2, 1) + pair(x1, 2)
        p0, p1, p2 = layer_classes(q0, q1, q2, q4, q5)
        result.append(p0 + lane_pair(p1, 1) + lane_pair(p2, 2))
    return result


def present(position, total, step):
    before = (position >= step).astype(jnp.float32)
    return before + (position + step < total).astype(jnp.float32)


def weight_tile(layer, layers, row, rows, depth):
    shape = (TALL, depth)
    sub = lax.broadcasted_iota(jnp.int32, shape, 0) + row
    spot = jnp.full(shape, layer, jnp.int32)
    nx1, nx2 = present(spot, layers, 1), present(spot, layers, 2)
    ny1, ny2 = present(sub, rows, 1), present(sub, rows, 2)
    one = jnp.ones(shape, jnp.float32)
    p0, p1, p2 = layer_classes(one, nx1 + ny1, nx1 * ny1, nx2 + ny2, nx2 * ny1 + nx1 * ny2)
    lane = lane_index(shape)
    return p0 + present(lane, depth, 1) * p1 + present(lane, depth, 2) * p2


def node_modes(ref, layer, row):
    result = []
    for comp in range(3):
        t = ref[comp, layer, pl.ds(row, SHORT + 8), :]
        depth, window = t.shape[-1], t.shape[0]
        tn = jnp.where(lane_index(t.shape) < depth - 1, pltpu.roll(t, depth - 1, 1), 0.0)
        s, d = t + tn, tn - t
        s0, d0 = s[0:SHORT], d[0:SHORT]
        s1, d1 = pltpu.roll(s, window - 1, 0)[0:SHORT], pltpu.roll(d, window - 1, 0)[0:SHORT]
        result.append((s0 + s1, d0 + d1, s1 - s0, d1 - d0))
    return result


def energy_tile(lower, upper):
    modes = []
    for a, b in zip(lower, upper):
        modes.append(
            {
                "x": b[0] - a[0],
                "z": a[1] + b[1],
                "y": a[2] + b[2],
                "yz": a[3] + b[3],
                "xz": b[1] - a[1],
                "xy": b[2] - a[2],
                "xyz": b[3] - a[3],
            }
        )
    u, v, w = modes
    sq = lambda t: t * t
    trace = sq(u["x"] + v["y"] + w["z"])
    linear = sq(v["xy"] + w["xz"]) + sq(u["xy"] + w["yz"]) + sq(u["xz"] + v["yz"])
    normal = sq(u["x"]) + sq(v["y"]) + sq(w["z"])
    bend = sq(u["xy"]) + sq(u["xz"]) + sq(v["xy"]) + sq(v["yz"]) + sq(w["yz"]) + sq(w["xz"])
    shear = sq(u["y"] + v["x"]) + sq(u["z"] + w["x"]) + sq(v["z"] + w["y"])
    twist = sq(u["yz"] + v["xz"]) + sq(u["yz"] + w["xy"]) + sq(v["xz"] + w["xy"])
    cubic = sq(u["xyz"]) + sq(v["xyz"]) + sq(w["xyz"])
    return (1.0 / 16.0) * (
        LAMBDA * trace
        + (LAMBDA / 3.0) * linear
        + (2.0 * SHEAR) * normal
        + SHEAR * (bend + shear)
        + (SHEAR / 3.0) * twist
        + ((LAMBDA + 4.0 * SHEAR) / 9.0) * cubic
    )


def kernel(
    ratio_in, density, void, fixed, disp, out,
    moved, fix, col_s, col_r, cor_s, cor_r, dens, dead, scale, energy, other, sens, mine, peer, ratio,
    local, send, recv,
):
    layers, rows, depth = density.shape
    half = layers // 2
    r, c, h = lax.axis_index("gz"), lax.axis_index("gy"), lax.axis_index("lc")
    nr, nc = lax.axis_size("gz"), lax.axis_size("gy")
    dz = 1 - 2 * h
    mid = pl.ds(8, rows)
    low, high = pl.ds(0, 8), pl.ds(rows + 8, 8)

    def there(step_z, step_y):
        z, y = r + step_z, c + step_y
        return (z >= 0) & (z < nr) & (y >= 0) & (y < nc)

    def remote(index, src, dst, step_z, step_y, core, arrival=None):
        copy = pltpu.make_async_remote_copy(
            src_ref=src, dst_ref=dst, send_sem=send.at[index],
            recv_sem=recv.at[index if arrival is None else arrival],
            device_id={"gz": r + step_z, "gy": c + step_y, "lc": core}, device_id_type=MESH,
        )
        goes, comes = there(step_z, step_y), there(-step_z, -step_y)
        return copy, goes, comes

    def between(index, src, dst, step_z, step_y, giver, taker):
        copy, goes, comes = remote(index, src, dst, step_z, step_y, taker)
        return copy, goes & (h == giver), comes & (h == taker)

    def flipped(index, src, dst, step_y):
        copy, goes, _ = remote(index, src, dst, -dz, step_y, 1 - h)
        return copy, goes, there(-dz, -step_y)

    def start(entry):
        copy, goes, _ = entry
        pl.when(goes)(copy.start)

    def arrive(entry):
        copy, _, comes = entry
        pl.when(comes)(copy.wait_recv)

    def left(entry):
        copy, goes, _ = entry
        pl.when(goes)(copy.wait_send)

    l0, b0 = half // 2 * (1 - h), half // 2 * h
    keep = half + 2
    lz, sb = (half + 2) * h, (layers - 2) * (1 - h)
    plane = pl.ds(0, rows)
    given, halo = (layers - 1) * (1 - h), (layers + 1) * h
    get_disp0 = pltpu.make_async_copy(disp.at[0, :, given], moved.at[:, given + 1, plane, :], local.at[0])
    get_fix0 = pltpu.make_async_copy(fixed.at[given], fix.at[given], local.at[1])
    get_disp = pltpu.make_async_copy(
        disp.at[0, :, pl.ds(h, layers - 1)], moved.at[:, pl.ds(h + 1, layers - 1), plane, :], local.at[2]
    )
    get_fix = pltpu.make_async_copy(
        fixed.at[pl.ds(h, layers - 1)], fix.at[pl.ds(h, layers - 1)], local.at[3]
    )
    get_dens = pltpu.make_async_copy(
        density.at[pl.ds(b0, keep)], dens.at[pl.ds(l0, keep), mid, :], local.at[4]
    )
    get_dead = pltpu.make_async_copy(void.at[pl.ds(half * h, half)], dead, local.at[5])
    get_ratio = pltpu.make_async_copy(ratio_in, ratio, local.at[6])
    for copy in (get_disp0, get_fix0, get_disp, get_fix, get_ratio, get_dens, get_dead):
        copy.start()

    barrier = pltpu.get_barrier_semaphore()
    for step_z in (-1, 0, 1):
        for step_y in (-1, 0, 1):
            for flip in (0, 1):
                if step_z == 0 and step_y == 0 and flip == 0:
                    continue
                core = h if flip == 0 else 1 - h

                @pl.when(there(step_z, step_y))
                def _():
                    pl.semaphore_signal(
                        barrier, inc=1,
                        device_id={"gz": r + step_z, "gy": c + step_y, "lc": core},
                        device_id_type=MESH,
                    )

    span_z = 1 + (r > 0).astype(jnp.int32) + (r < nr - 1).astype(jnp.int32)
    span_y = 1 + (c > 0).astype(jnp.int32) + (c < nc - 1).astype(jnp.int32)

    own, edge = pl.ds(b0, keep), pl.ds(sb, 2)
    top, bottom = pl.ds(rows - 8, 8), pl.ds(0, 8)
    near, far = pl.ds(l0, keep), pl.ds(lz, 2)
    dens_rows = [
        remote(1, density.at[own, top, :], dens.at[near, low, :], 0, 1, h),
        remote(2, density.at[own, bottom, :], dens.at[near, high, :], 0, -1, h),
    ]
    dens_far = [
        remote(0, density.at[edge], dens.at[far, mid, :], dz, 0, h),
        remote(3, density.at[edge, top, :], dens.at[far, low, :], dz, 1, h),
        remote(4, density.at[edge, bottom, :], dens.at[far, high, :], dz, -1, h),
    ]

    def free_layer(i):
        free = (1 - fix[i]).astype(jnp.float32)
        for comp in range(3):
            moved[comp, i + 1, plane, :] = moved[comp, i + 1, plane, :] * free

    send_disp = remote(5, moved.at[:, given + 1, plane, :], moved.at[:, halo, plane, :], dz, 0, h)
    send_col = remote(6, col_s, col_r, 0, -1, h)
    send_cor = remote(7, cor_s, cor_r, dz, -1, h)
    get_disp0.wait()
    get_fix0.wait()
    free_layer(given)
    for comp in range(3):
        cor_s[comp : comp + 1, :] = moved[comp, given + 1, 0:1, :]
    pl.semaphore_wait(barrier, 2 * span_z * span_y - 1)
    start(send_cor)
    for entry in [send_disp, *dens_rows, *dens_far]:
        start(entry)
    get_disp.wait()
    get_fix.wait()

    def free_other(i, _):
        free_layer(i + h)
        return 0

    lax.fori_loop(0, layers - 1, free_other, 0)
    for comp in range(3):
        for i in range(layers):
            col_s[comp, i : i + 1, :] = moved[comp, i + 1, 0:1, :]
    start(send_col)

    blank = jnp.zeros((8, depth), jnp.float32)

    @pl.when(r == nr - 1)
    def _():
        for comp in range(3):
            moved[comp, layers + 1, plane, :] = jnp.zeros((rows, depth), jnp.float32)
            moved[comp, layers + 1, pl.ds(rows, 8), :] = blank

    @pl.when(c == nc - 1)
    def _():
        col_r[...] = jnp.zeros_like(col_r)

    @pl.when(jnp.logical_not(there(-dz, 1)))
    def _():
        cor_r[...] = jnp.zeros_like(cor_r)

    @pl.when(c == 0)
    def _():
        mine[low, :] = blank
        peer[low, :] = blank

    @pl.when(c == nc - 1)
    def _():
        mine[high, :] = blank
        peer[high, :] = blank

    for ref in (dens, sens):

        @pl.when(c == 0)
        def _():
            for i in range(half + 4):
                ref[i, low, :] = blank

        @pl.when(c == nc - 1)
        def _():
            for i in range(half + 4):
                ref[i, high, :] = blank

        @pl.when(jnp.logical_not(there(-dz, 0)))
        def _():
            for i in range(2):
                ref[lz + i] = jnp.zeros((rows + 16, depth), jnp.float32)

    get_ratio.wait()
    ratio_sum = ratio[0]
    for case in range(1, ratio.shape[0]):
        ratio_sum = ratio_sum + ratio[case]
    total = jnp.full((8, depth), ratio_sum.astype(jnp.float32))
    share = jnp.full((8, depth), ratio[h].astype(jnp.float32)) / total

    tiles = rows // SHORT

    def energy_rows(first, count, j):
        row = pl.multiple_of(j * SHORT, SHORT)
        lower = node_modes(moved, first + 1, row)
        for k in range(count):
            upper = node_modes(moved, first + k + 2, row)
            energy[first + k, pl.ds(row, SHORT), :] = share * energy_tile(lower, upper)
            lower = upper

    def energy_layers(first, count, end):
        def tile(j, _):
            energy_rows(first, count, j)
            return 0

        lax.fori_loop(0, end, tile, 0)

    give = half * (1 - h)
    swap_a = remote(
        8, energy.at[pl.ds(give, half - 1)], other.at[pl.ds(0, half - 1)], 0, 0, 1 - h
    )
    swap_b = between(
        9, energy.at[pl.ds(half - 1, 1)], other.at[pl.ds(half - 1, 1)], 0, 0, 1, 0
    )
    energy_layers(give, half - 1, tiles - 1)
    arrive(send_col)
    for comp in range(3):
        for i in range(layers):
            moved[comp, i + 1, pl.ds(rows, 1), :] = col_r[comp, i : i + 1, :]
    energy_rows(give, half - 1, tiles - 1)
    start(swap_a)
    energy_layers((half - 1) * h, half, tiles)
    start(swap_b)

    close, wide = 2 * (1 - h), 2 * h

    def scale_two(j):
        def tile(k, _):
            row = pl.multiple_of(k * TALL, TALL)
            cones = cone_tiles(dens, j, row, 2)
            for n in range(2):
                weights = weight_tile(
                    r * layers + half * h + j + n, nr * layers, c * rows + row, nc * rows, depth
                )
                inverse = 1.0 / weights
                physical = cones[n] * inverse
                alive = (1 - dead[j + n, pl.ds(row, TALL), :]).astype(jnp.float32)
                scale[j + n, pl.ds(row, TALL), :] = (
                    alive * (-3.0 * (1.0 - 0.001)) * physical * physical * inverse
                )
            return 0

        lax.fori_loop(0, rows // TALL, tile, 0)

    def sense(j):
        sens[2 + j, mid, :] = scale[j] * (energy[half * h + j] + other[j])

    get_dens.wait()
    get_dead.wait()
    for entry in dens_rows:
        arrive(entry)
    scale_two(close)
    arrive(swap_a)
    arrive(swap_b)
    sense(close)
    sense(close + 1)

    ps, pd = pl.ds(half - (half - 2) * h, 2), pl.ds((half + 2) * h, 2)
    zs, zd = pl.ds(2 + (half - 2) * h, 2), pl.ds((half + 2) * (1 - h), 2)
    last, first = pl.ds(rows, 8), pl.ds(8, 8)
    close_copies = [
        remote(10, sens.at[ps, mid, :], sens.at[pd, mid, :], 0, 0, 1 - h),
        remote(12, sens.at[ps, last, :], sens.at[ps, low, :], 0, 1, h),
        remote(13, sens.at[ps, first, :], sens.at[ps, high, :], 0, -1, h),
        remote(14, sens.at[ps, last, :], sens.at[pd, low, :], 0, 1, 1 - h),
        remote(15, sens.at[ps, first, :], sens.at[pd, high, :], 0, -1, 1 - h),
    ]
    for entry in close_copies:
        start(entry)

    wide_copies = [
        flipped(16, sens.at[zs, last, :], sens.at[zd, low, :], 1),
        flipped(17, sens.at[zs, first, :], sens.at[zd, high, :], -1),
        flipped(11, sens.at[zs, mid, :], sens.at[zd, mid, :], 0),
    ]
    row_copies = [
        remote(18, sens.at[zs, last, :], sens.at[zs, low, :], 0, 1, h),
        remote(19, sens.at[zs, first, :], sens.at[zs, high, :], 0, -1, h),
    ]
    edge_copies = [
        remote(21, mine.at[last, :], mine.at[low, :], 0, 1, h),
        remote(22, mine.at[first, :], mine.at[high, :], 0, -1, h),
        flipped(23, mine.at[last, :], peer.at[low, :], 1),
        flipped(24, mine.at[first, :], peer.at[high, :], -1),
        flipped(20, mine.at[mid, :], peer.at[mid, :], 0),
    ]
    atop = (r == nr - 1) & (h == 0)
    whole = energy.at[layers - 1]
    top_copies = [
        remote(27, whole.at[plane, :], peer.at[mid, :], 0, 0, 1, 20),
        remote(25, whole.at[top, :], peer.at[low, :], 0, 1, 1, 23),
        remote(26, whole.at[bottom, :], peer.at[high, :], 0, -1, 1, 24),
    ]
    top_copies = [
        (copy, goes & atop, comes & (r == nr - 1) & (h == 1)) for copy, goes, comes in top_copies
    ]
    joined = (h == 1) | (r > 0)
    edge_copies[:2] = [(copy, goes & joined, comes & joined) for copy, goes, comes in edge_copies[:2]]
    arrivals = [top_copies[1], top_copies[2], top_copies[0]]
    arrivals = [
        (copy, goes, comes | extra)
        for (copy, goes, comes), (_, _, extra) in zip(edge_copies[2:], arrivals)
    ]

    def boundary():
        @pl.when(atop)
        def _():
            energy_layers(layers - 1, 1, tiles)

        for entry in top_copies:
            start(entry)
        arrive(send_disp)
        arrive(send_cor)
        for comp in range(3):
            moved[comp, halo, pl.ds(rows, 1), :] = cor_r[comp : comp + 1, :]

        @pl.when(joined)
        def _():
            def tile(k, _):
                row = pl.multiple_of(k * SHORT, SHORT)
                here = pl.multiple_of(k * SHORT + 8, SHORT)
                mine[pl.ds(here, SHORT), :] = share * energy_tile(
                    node_modes(moved, layers * h, row), node_modes(moved, layers * h + 1, row)
                )
                return 0

            lax.fori_loop(0, tiles, tile, 0)
        for entry in edge_copies:
            start(entry)

    def spread():
        for entry in dens_far:
            arrive(entry)
        scale_two(wide)
        sense(wide)

        @pl.when(h == 0)
        def _():
            sense(1)

        @pl.when(h == 1)
        def _():
            sens[half + 1, mid, :] = scale[half - 1]

        for entry in wide_copies + row_copies:
            start(entry)

    boundary()
    spread()

    def filter_layers(j, count):
        def tile(k, _):
            row = pl.multiple_of(k * TALL, TALL)
            cones = cone_tiles(sens, j, row, count)
            for n in range(count):
                alive = (1 - dead[j + n, pl.ds(row, TALL), :]).astype(jnp.float32)
                out[half * h + j + n, pl.ds(row, TALL), :] = alive * cones[n]
            return 0

        lax.fori_loop(0, rows // TALL, tile, 0)

    def hand_over(index, giver, j, count):
        place = pl.ds(half * giver + j, count)
        return between(index, out.at[place], out.at[place], 0, 0, giver, 1 - giver)

    early = [hand_over(28, 0, 2, half - 2), hand_over(29, 1, 0, half - 3)]
    late = [hand_over(30, 0, 0, 2), hand_over(31, 1, half - 3, 3)]
    for entry in close_copies:
        arrive(entry)
    for entry in row_copies:
        arrive(entry)

    @pl.when(h == 0)
    def _():
        filter_layers(2, half - 2)

    @pl.when(h == 1)
    def _():
        filter_layers(0, half - 3)

    for entry in early:
        start(entry)
    for entry in wide_copies:
        arrive(entry)
    for entry in wide_copies + row_copies:
        left(entry)
    for entry in edge_copies[:2] + arrivals:
        arrive(entry)

    @pl.when(joined)
    def _():
        b = 1 + half * h
        sens[b] = sens[b] * (mine[...] + peer[...])

    @pl.when(h == 0)
    def _():
        filter_layers(0, 2)

    @pl.when(h == 1)
    def _():
        filter_layers(half - 3, 3)

    for entry in late:
        start(entry)
    sent = [*dens_rows, *dens_far, send_disp, send_col, send_cor, swap_a, swap_b]
    for entry in sent + close_copies + edge_copies + top_copies + early + late:
        left(entry)
    for entry in early + late:
        arrive(entry)


def shards(density, void_mask, fixed_mask, displacement, load_ratio):
    layers, rows, depth = density.shape
    half = layers // 2
    f32 = jnp.float32
    hbm = pl.BlockSpec(memory_space=pl.ANY)
    return pl.pallas_call(
        kernel,
        out_shape=pltpu.VMEM(density.shape, f32),
        in_specs=[hbm] * 5,
        out_specs=pl.BlockSpec(memory_space=pltpu.VMEM),
        scratch_shapes=[
            pltpu.VMEM((3, layers + 2, rows + 8, depth), f32),
            pltpu.VMEM((layers, rows, depth), jnp.int32),
            pltpu.VMEM((3, layers, depth), f32),
            pltpu.VMEM((3, layers, depth), f32),
            pltpu.VMEM((8, depth), f32),
            pltpu.VMEM((8, depth), f32),
            pltpu.VMEM((half + 4, rows + 16, depth), f32),
            pltpu.VMEM((half, rows, depth), jnp.int32),
            pltpu.VMEM((half, rows, depth), f32),
            pltpu.VMEM((layers, rows, depth), f32),
            pltpu.VMEM((half, rows, depth), f32),
            pltpu.VMEM((half + 4, rows + 16, depth), f32),
            pltpu.VMEM((rows + 16, depth), f32),
            pltpu.VMEM((rows + 16, depth), f32),
            pltpu.SMEM(load_ratio.shape, load_ratio.dtype),
            pltpu.SemaphoreType.DMA((7,)),
            pltpu.SemaphoreType.DMA((N_COPIES,)),
            pltpu.SemaphoreType.DMA((N_COPIES,)),
        ],
        compiler_params=pltpu.CompilerParams(collective_id=0, has_side_effects=True),
    )(load_ratio, density, void_mask, fixed_mask, displacement)


def solution(mesh):
    placed = (
        P(("parts", "gz"), "gy", None),
        P(("parts", "gz"), "gy", None),
        P(("parts", "gz"), "gy", None),
        P("lc", None, ("parts", "gz"), "gy", None),
        P("parts"),
    )
    return jax.shard_map(
        shards,
        mesh=mesh,
        in_specs=placed,
        out_specs=P(("parts", "gz"), "gy", None),
        check_vma=False,
    )
```

```python
import math

import jax
import jax.numpy as jnp
from jax import lax
from jax.experimental import pallas as pl
from jax.experimental.pallas import tpu as pltpu
from jax.sharding import PartitionSpec as P

MESH = pl.DeviceIdType.MESH
POISSON = 0.3
FACTOR = 1.0 / ((1.0 + POISSON) * (1.0 - 2.0 * POISSON))
LAMBDA = POISSON * FACTOR
SHEAR = (0.5 - POISSON) * FACTOR
RATIO = LAMBDA / SHEAR
W = [2.5 - math.sqrt(d) for d in range(7)]
CHUNKS = 2
N_SEND = 23
N_RECV = 32
TALL = 32
SHORT = 8


def layer_classes(q0, q1, q2, q4, q5):
    p0 = W[0] * q0 + W[1] * q1 + W[2] * q2 + W[4] * q4 + W[5] * q5
    p1 = W[1] * q0 + W[2] * q1 + W[3] * q2 + W[5] * q4 + W[6] * q5
    p2 = W[4] * q0 + W[5] * q1 + W[6] * q2
    return p0, p1, p2


def lane_index(shape):
    return lax.broadcasted_iota(jnp.int32, shape, len(shape) - 1)


def lane_pair(field, step):
    depth = field.shape[-1]
    lane = lane_index(field.shape)
    after = jnp.where(lane < depth - step, pltpu.roll(field, depth - step, 1), 0.0)
    before = jnp.where(lane >= step, pltpu.roll(field, step, 1), 0.0)
    return after + before


def cone_tiles(ref, layer, row, count):
    window = TALL + 16
    f = [ref[layer + k, pl.ds(row, window), :] for k in range(count + 4)]
    mid = slice(8, 8 + TALL)

    def pair(t, step):
        return (pltpu.roll(t, step, 0) + pltpu.roll(t, window - step, 0))[mid]

    result = []
    for k in range(count):
        x0, x1, x2 = f[k + 2], f[k + 1] + f[k + 3], f[k] + f[k + 4]
        q0 = x0[mid]
        q1 = x1[mid] + pair(x0, 1)
        q2 = pair(x1, 1)
        q4 = x2[mid] + pair(x0, 2)
        q5 = pair(x2, 1) + pair(x1, 2)
        p0, p1, p2 = layer_classes(q0, q1, q2, q4, q5)
        result.append(p0 + lane_pair(p1, 1) + lane_pair(p2, 2))
    return result


def present(position, total, step):
    before = (position >= step).astype(jnp.float32)
    return before + (position + step < total).astype(jnp.float32)


def weight_tile(layer, layers, row, rows, depth):
    shape = (TALL, depth)
    sub = lax.broadcasted_iota(jnp.int32, shape, 0) + row
    spot = jnp.full(shape, layer, jnp.int32)
    nx1, nx2 = present(spot, layers, 1), present(spot, layers, 2)
    ny1, ny2 = present(sub, rows, 1), present(sub, rows, 2)
    one = jnp.ones(shape, jnp.float32)
    p0, p1, p2 = layer_classes(one, nx1 + ny1, nx1 * ny1, nx2 + ny2, nx2 * ny1 + nx1 * ny2)
    lane = lane_index(shape)
    return p0 + present(lane, depth, 1) * p1 + present(lane, depth, 2) * p2


def node_modes(ref, layer, row):
    result = []
    for comp in range(3):
        t = ref[comp, layer, pl.ds(row, SHORT + 8), :]
        depth, window = t.shape[-1], t.shape[0]
        here, after = t[0:SHORT], pltpu.roll(t, window - 1, 0)[0:SHORT]
        s, d = here + after, after - here
        inner = lane_index(s.shape) < depth - 1
        sn = jnp.where(inner, pltpu.roll(s, depth - 1, 1), 0.0)
        dn = jnp.where(inner, pltpu.roll(d, depth - 1, 1), 0.0)
        result.append((s + sn, sn - s, d + dn, dn - d))
    return result


def energy_tile(lower, upper):
    modes = []
    for a, b in zip(lower, upper):
        modes.append(
            {
                "x": b[0] - a[0],
                "z": a[1] + b[1],
                "y": a[2] + b[2],
                "yz": a[3] + b[3],
                "xz": b[1] - a[1],
                "xy": b[2] - a[2],
                "xyz": b[3] - a[3],
            }
        )
    u, v, w = modes
    sq = lambda t: t * t
    trace = sq(u["x"] + v["y"] + w["z"])
    normal = sq(u["x"]) + sq(v["y"]) + sq(w["z"])
    bend = sq(u["xy"]) + sq(u["xz"]) + sq(v["xy"]) + sq(v["yz"]) + sq(w["yz"]) + sq(w["xz"])
    cross = v["xy"] * w["xz"] + u["xy"] * w["yz"] + u["xz"] * v["yz"]
    shear = sq(u["y"] + v["x"]) + sq(u["z"] + w["x"]) + sq(v["z"] + w["y"])
    pair = v["xz"] + w["xy"]
    twist = u["yz"] * (u["yz"] + pair) + v["xz"] * pair + sq(w["xy"])
    cubic = sq(u["xyz"]) + sq(v["xyz"]) + sq(w["xyz"])
    return (
        RATIO * trace
        + 2.0 * normal
        + (1.0 + RATIO / 3.0) * bend
        + (2.0 * RATIO / 3.0) * cross
        + shear
        + (2.0 / 3.0) * twist
        + ((RATIO + 4.0) / 9.0) * cubic
    )


def kernel(
    ratio_in, density, void, fixed, disp, out,
    moved, fix, col_s, col_r, cor_s, cor_r, dens, dead, scale, energy, other, sens, mine, peer, ratio,
    local, send, recv, ready,
):
    layers, rows, depth = density.shape
    half = layers // 2
    r, c, h = lax.axis_index("gz"), lax.axis_index("gy"), lax.axis_index("lc")
    nr, nc = lax.axis_size("gz"), lax.axis_size("gy")
    dz = 1 - 2 * h
    mid = pl.ds(8, rows)
    low, high = pl.ds(0, 8), pl.ds(rows + 8, 8)

    def there(step_z, step_y):
        z, y = r + step_z, c + step_y
        return (z >= 0) & (z < nr) & (y >= 0) & (y < nc)

    def remote(index, src, dst, step_z, step_y, core, slot=None):
        copy = pltpu.make_async_remote_copy(
            src_ref=src, dst_ref=dst, send_sem=send.at[index if slot is None else slot],
            recv_sem=recv.at[index],
            device_id={"gz": r + step_z, "gy": c + step_y, "lc": core}, device_id_type=MESH,
        )
        goes, comes = there(step_z, step_y), there(-step_z, -step_y)
        return copy, goes, comes

    def between(index, src, dst, giver, slot=None):
        taker = 1 - giver
        copy, goes, comes = remote(index, src, dst, 0, 0, taker, slot)
        return copy, goes & (h == giver), comes & (h == taker)

    def flipped(index, src, dst, step_y, slot=None):
        copy, goes, _ = remote(index, src, dst, -dz, step_y, 1 - h, slot)
        return copy, goes, there(-dz, -step_y)

    def start(entry, when=True):
        copy, goes, _ = entry
        pl.when(goes & when)(copy.start)

    def arrive(entry):
        copy, _, comes = entry
        pl.when(comes)(copy.wait_recv)

    def left(entry):
        copy, goes, _ = entry
        pl.when(goes)(copy.wait_send)

    l0, b0 = half // 2 * (1 - h), half // 2 * h
    keep = half + 2
    lz, sb = (half + 2) * h, (layers - 2) * (1 - h)
    plane = pl.ds(0, rows)
    given, halo = (layers - 1) * (1 - h), (layers + 1) * h
    get_disp0 = pltpu.make_async_copy(disp.at[0, :, given], moved.at[:, given + 1, plane, :], local.at[0])
    get_fix0 = pltpu.make_async_copy(fixed.at[given], fix.at[given], local.at[1])
    get_disp = pltpu.make_async_copy(
        disp.at[0, :, pl.ds(h, layers - 1)], moved.at[:, pl.ds(h + 1, layers - 1), plane, :], local.at[2]
    )
    get_fix = pltpu.make_async_copy(
        fixed.at[pl.ds(h, layers - 1)], fix.at[pl.ds(h, layers - 1)], local.at[3]
    )
    get_dens = pltpu.make_async_copy(
        density.at[pl.ds(b0, keep)], dens.at[pl.ds(l0, keep), mid, :], local.at[4]
    )
    get_dead = pltpu.make_async_copy(void.at[pl.ds(half * h, half)], dead, local.at[5])
    get_ratio = pltpu.make_async_copy(ratio_in, ratio, local.at[6])
    for copy in (get_disp0, get_fix0, get_disp, get_fix, get_ratio, get_dens, get_dead):
        copy.start()

    barrier = pltpu.get_barrier_semaphore()
    def greet(semaphore, step_z, step_y, core):
        @pl.when(there(step_z, step_y))
        def _():
            pl.semaphore_signal(
                semaphore, inc=1,
                device_id={"gz": r + step_z, "gy": c + step_y, "lc": core},
                device_id_type=MESH,
            )

    flag = lambda held: held.astype(jnp.int32)

    def await_from(semaphore, step_z, step_y, count):
        @pl.when(there(step_z, step_y))
        def _():
            pl.semaphore_wait(semaphore, count)

    for core in (h, 1 - h):
        greet(barrier, 1, 0, core)
        greet(barrier, 0, 1, core)
    greet(barrier, 0, 0, 1 - h)

    own, edge = pl.ds(b0, keep), pl.ds(sb, 2)
    top, bottom = pl.ds(rows - 8, 8), pl.ds(0, 8)
    near, far = pl.ds(l0, keep), pl.ds(lz, 2)
    dens_rows = [
        remote(1, density.at[own, top, :], dens.at[near, low, :], 0, 1, h),
        remote(2, density.at[own, bottom, :], dens.at[near, high, :], 0, -1, h),
    ]
    dens_far = [
        remote(0, density.at[edge], dens.at[far, mid, :], dz, 0, h),
        remote(3, density.at[edge, top, :], dens.at[far, low, :], dz, 1, h),
        remote(4, density.at[edge, bottom, :], dens.at[far, high, :], dz, -1, h),
    ]

    def free_layer(i):
        free = (1 - fix[i]).astype(jnp.float32)
        for comp in range(3):
            moved[comp, i + 1, plane, :] = moved[comp, i + 1, plane, :] * free

    tall = rows // CHUNKS
    parts = [pl.ds(q * tall, tall) for q in range(CHUNKS)]
    send_disp = [
        remote(5 + q, moved.at[:, given + 1, part, :], moved.at[:, halo, part, :], dz, 0, h)
        for q, part in enumerate(parts)
    ]
    send_col = remote(7, col_s, col_r, 0, -1, h)
    send_cor = remote(8, cor_s, cor_r, dz, -1, h)
    pl.semaphore_wait(barrier, 2 * (flag(r > 0) + flag(c > 0)) + 1)
    for core in (h, 1 - h):
        greet(ready.at[0], -1, 0, core)
        greet(ready.at[1], 0, -1, core)
    start(dens_far[0], h == 1)
    start(dens_rows[1])
    get_disp0.wait()
    get_fix0.wait()
    free_layer(given)
    for comp in range(3):
        cor_s[comp : comp + 1, :] = moved[comp, given + 1, 0:1, :]
    get_disp.wait()
    get_fix.wait()

    def free_other(i, _):
        free_layer(i + h)
        return 0

    lax.fori_loop(0, layers - 1, free_other, 0)
    for comp in range(3):
        for i in range(layers):
            col_s[comp, i : i + 1, :] = moved[comp, i + 1, 0:1, :]
    start(send_col)
    await_from(ready.at[0], 1, 0, 2)
    start(dens_far[0], h == 0)
    await_from(ready.at[1], 0, 1, 2)
    start(dens_rows[0])
    for step_y in (-1, 1):
        greet(ready.at[2], 0, step_y, h)

    get_ratio.wait()
    ratio_sum = ratio[0]
    for case in range(1, ratio.shape[0]):
        ratio_sum = ratio_sum + ratio[case]
    total = jnp.full((8, depth), ratio_sum.astype(jnp.float32))
    share = (SHEAR / 16.0) * (jnp.full((8, depth), ratio[h].astype(jnp.float32)) / total)

    tiles = rows // SHORT

    def energy_rows(first, count, j):
        row = pl.multiple_of(j * SHORT, SHORT)
        lower = node_modes(moved, first + 1, row)
        for k in range(count):
            upper = node_modes(moved, first + k + 2, row)
            energy[first + k, pl.ds(row, SHORT), :] = share * energy_tile(lower, upper)
            lower = upper

    def energy_layers(first, count, begin, end):
        def tile(j, _):
            energy_rows(first, count, begin + 2 * j)
            energy_rows(first, count, begin + 2 * j + 1)
            return 0

        lax.fori_loop(0, (end - begin) // 2, tile, 0)

    give = half * (1 - h)
    head = (tiles - 2) * SHORT
    swap_rows = [pl.ds(0, head), pl.ds(head, rows - head)]
    swap_a = [
        remote(
            9 + q, energy.at[pl.ds(give, half - 1), part, :],
            other.at[pl.ds(0, half - 1), part, :], 0, 0, 1 - h,
        )
        for q, part in enumerate(swap_rows)
    ]
    swap_b = [
        between(11 + q, energy.at[half - 1, part, :], other.at[half - 1, part, :], 1)
        for q, part in enumerate(swap_rows)
    ]
    rest = (half - 1) * h
    energy_layers(give, half - 1, 0, tiles - 2)
    start(swap_a[0])
    await_from(ready.at[2], 0, -1, 1)
    await_from(ready.at[2], 0, 1, 1)
    for entry in [*dens_far[1:], send_cor, *send_disp[::-1]]:
        start(entry)
    energy_layers(rest, half, 0, tiles - 2)
    start(swap_b[0])

    blank = jnp.zeros((8, depth), jnp.float32)

    @pl.when(r == nr - 1)
    def _():
        for comp in range(3):
            moved[comp, layers + 1, plane, :] = jnp.zeros((rows, depth), jnp.float32)
            moved[comp, layers + 1, pl.ds(rows, 8), :] = blank

    @pl.when(c == nc - 1)
    def _():
        col_r[...] = jnp.zeros_like(col_r)

    @pl.when(jnp.logical_not(there(-dz, 1)))
    def _():
        cor_r[...] = jnp.zeros_like(cor_r)

    @pl.when(c == 0)
    def _():
        mine[low, :] = blank
        peer[low, :] = blank

    @pl.when(c == nc - 1)
    def _():
        mine[high, :] = blank
        peer[high, :] = blank

    for ref in (dens, sens):

        @pl.when(c == 0)
        def _():
            for i in range(half + 4):
                ref[i, low, :] = blank

        @pl.when(c == nc - 1)
        def _():
            for i in range(half + 4):
                ref[i, high, :] = blank

        @pl.when(jnp.logical_not(there(-dz, 0)))
        def _():
            for i in range(2):
                ref[lz + i] = jnp.zeros((rows + 16, depth), jnp.float32)

    arrive(send_col)
    for comp in range(3):
        for i in range(layers):
            moved[comp, i + 1, pl.ds(rows, 1), :] = col_r[comp, i : i + 1, :]
    energy_layers(give, half - 1, tiles - 2, tiles)
    start(swap_a[1])
    energy_layers(rest, half, tiles - 2, tiles)
    start(swap_b[1])

    close, wide = 2 * (1 - h), 2 * h

    def scale_two(j):
        def tile(k, _):
            row = pl.multiple_of(k * TALL, TALL)
            cones = cone_tiles(dens, j, row, 2)
            for n in range(2):
                weights = weight_tile(
                    r * layers + half * h + j + n, nr * layers, c * rows + row, nc * rows, depth
                )
                inverse = 1.0 / weights
                physical = cones[n] * inverse
                alive = (1 - dead[j + n, pl.ds(row, TALL), :]).astype(jnp.float32)
                scale[j + n, pl.ds(row, TALL), :] = (
                    alive * (-3.0 * (1.0 - 0.001)) * physical * physical * inverse
                )
            return 0

        lax.fori_loop(0, rows // TALL, tile, 0)

    def sense(j):
        sens[2 + j, mid, :] = scale[j] * (energy[half * h + j] + other[j])

    get_dens.wait()
    get_dead.wait()
    for entry in dens_rows:
        arrive(entry)
    scale_two(close)
    for entry in swap_a + swap_b:
        arrive(entry)
    sense(close)
    sense(close + 1)

    ps, pd = pl.ds(half - (half - 2) * h, 2), pl.ds((half + 2) * h, 2)
    zs, zd = pl.ds(2 + (half - 2) * h, 2), pl.ds((half + 2) * (1 - h), 2)
    last, first = pl.ds(rows, 8), pl.ds(8, 8)
    close_copies = [
        remote(13, sens.at[ps, mid, :], sens.at[pd, mid, :], 0, 0, 1 - h),
        remote(14, sens.at[ps, last, :], sens.at[ps, low, :], 0, 1, h),
        remote(15, sens.at[ps, first, :], sens.at[ps, high, :], 0, -1, h),
        remote(16, sens.at[ps, last, :], sens.at[pd, low, :], 0, 1, 1 - h),
        remote(17, sens.at[ps, first, :], sens.at[pd, high, :], 0, -1, 1 - h),
    ]
    for entry in close_copies:
        start(entry)

    wide_copies = [
        flipped(18, sens.at[zs, last, :], sens.at[zd, low, :], 1),
        flipped(19, sens.at[zs, first, :], sens.at[zd, high, :], -1),
        flipped(20, sens.at[zs, mid, :], sens.at[zd, mid, :], 0),
    ]
    row_copies = [
        remote(21, sens.at[zs, last, :], sens.at[zs, low, :], 0, 1, h),
        remote(22, sens.at[zs, first, :], sens.at[zs, high, :], 0, -1, h),
    ]
    edge_copies = [
        remote(23, mine.at[last, :], mine.at[low, :], 0, 1, h, 0),
        remote(24, mine.at[first, :], mine.at[high, :], 0, -1, h, 1),
        flipped(25, mine.at[last, :], peer.at[low, :], 1, 2),
        flipped(26, mine.at[first, :], peer.at[high, :], -1, 3),
    ]
    main_copies = [
        flipped(27 + q, mine.at[pl.ds(8 + q * tall, tall), :], peer.at[pl.ds(8 + q * tall, tall), :], 0, 4 + q)
        for q in range(CHUNKS)
    ]
    atop = (r == nr - 1) & (h == 0)
    whole = energy.at[layers - 1]
    top_copies = [
        remote(25, whole.at[top, :], peer.at[low, :], 0, 1, 1, 6),
        remote(26, whole.at[bottom, :], peer.at[high, :], 0, -1, 1, 7),
        remote(27, whole.at[parts[0], :], peer.at[pl.ds(8, tall), :], 0, 0, 1, 8),
        remote(28, whole.at[parts[1], :], peer.at[pl.ds(8 + tall, tall), :], 0, 0, 1, 9),
    ]
    top_copies = [
        (copy, goes & atop, comes & (r == nr - 1) & (h == 1)) for copy, goes, comes in top_copies
    ]
    joined = (h == 1) | (r > 0)
    edge_copies[:2] = [(copy, goes & joined, comes & joined) for copy, goes, comes in edge_copies[:2]]
    arrivals = [
        (copy, goes, comes | extra)
        for (copy, goes, comes), (_, _, extra) in zip(edge_copies[2:] + main_copies, top_copies)
    ]
    pieces = [
        [edge_copies[1], edge_copies[3], main_copies[0]],
        [edge_copies[0], edge_copies[2], main_copies[1]],
    ]

    def boundary():
        for entry in [*dens_rows, *dens_far, *send_disp, send_col, send_cor, *swap_a, *swap_b]:
            left(entry)

        @pl.when(atop)
        def _():
            energy_layers(layers - 1, 1, 0, tiles)

        for entry in top_copies:
            start(entry)
        arrive(send_cor)
        for comp in range(3):
            moved[comp, halo, pl.ds(rows, 1), :] = cor_r[comp : comp + 1, :]
        for q in reversed(range(CHUNKS)):
            arrive(send_disp[q])

            @pl.when(joined)
            def _():
                for n in range(tall // SHORT):
                    row = q * tall + n * SHORT
                    mine[pl.ds(row + 8, SHORT), :] = share * energy_tile(
                        node_modes(moved, layers * h, row), node_modes(moved, layers * h + 1, row)
                    )

            for entry in pieces[q]:
                start(entry)

    def spread():
        for entry in dens_far:
            arrive(entry)
        scale_two(wide)
        sense(wide)

        @pl.when(h == 0)
        def _():
            sense(1)

        @pl.when(h == 1)
        def _():
            sens[half + 1, mid, :] = scale[half - 1]

        for entry in wide_copies + row_copies:
            start(entry)

    spread()
    boundary()

    def filter_rows(j, count, row):
        cones = cone_tiles(sens, j, row, count)
        for n in range(count):
            alive = (1 - dead[j + n, pl.ds(row, TALL), :]).astype(jnp.float32)
            out[half * h + j + n, pl.ds(row, TALL), :] = alive * cones[n]

    def filter_layers(j, count):
        def tile(k, _):
            filter_rows(j, count, pl.multiple_of(k * TALL, TALL))
            return 0

        lax.fori_loop(0, rows // TALL, tile, 0)

    def hand_over(index, giver, j, count, part):
        place = out.at[pl.ds(half * giver + j, count), part, :]
        return between(index, place, place, giver, index - 19)

    early = [hand_over(29, 0, 2, half - 2, plane), hand_over(29, 1, 0, half - 3, plane)]
    strips = [pl.ds(k * TALL, TALL) for k in range(rows // TALL)]
    late = [
        [hand_over(30 + k, 0, 0, 2, strip), hand_over(30 + k, 1, half - 3, 3, strip)]
        for k, strip in enumerate(strips)
    ]
    for entry in close_copies + row_copies:
        arrive(entry)

    @pl.when(h == 0)
    def _():
        filter_layers(2, half - 2)

    @pl.when(h == 1)
    def _():
        filter_layers(0, half - 3)

    for entry in early:
        start(entry)
    for entry in close_copies + row_copies:
        left(entry)
    for entry in wide_copies:
        arrive(entry)
    for entry in wide_copies:
        left(entry)
    for entry in edge_copies + main_copies + top_copies + early:
        left(entry)
    for entry in edge_copies[:2] + arrivals:
        arrive(entry)

    @pl.when(joined)
    def _():
        b = 1 + half * h
        sens[b] = sens[b] * (mine[...] + peer[...])

    for k in range(rows // TALL):

        @pl.when(h == 0)
        def _():
            filter_rows(0, 2, k * TALL)

        @pl.when(h == 1)
        def _():
            filter_rows(half - 3, 3, k * TALL)

        for entry in late[k]:
            start(entry)
    late = [entry for pair in late for entry in pair]
    for entry in late:
        left(entry)
    for entry in early + late:
        arrive(entry)


def shards(density, void_mask, fixed_mask, displacement, load_ratio):
    layers, rows, depth = density.shape
    half = layers // 2
    f32 = jnp.float32
    hbm = pl.BlockSpec(memory_space=pl.ANY)
    return pl.pallas_call(
        kernel,
        out_shape=pltpu.VMEM(density.shape, f32),
        in_specs=[hbm] * 5,
        out_specs=pl.BlockSpec(memory_space=pltpu.VMEM),
        scratch_shapes=[
            pltpu.VMEM((3, layers + 2, rows + 8, depth), f32),
            pltpu.VMEM((layers, rows, depth), jnp.int32),
            pltpu.VMEM((3, layers, depth), f32),
            pltpu.VMEM((3, layers, depth), f32),
            pltpu.VMEM((8, depth), f32),
            pltpu.VMEM((8, depth), f32),
            pltpu.VMEM((half + 4, rows + 16, depth), f32),
            pltpu.VMEM((half, rows, depth), jnp.int32),
            pltpu.VMEM((half, rows, depth), f32),
            pltpu.VMEM((layers, rows, depth), f32),
            pltpu.VMEM((half, rows, depth), f32),
            pltpu.VMEM((half + 4, rows + 16, depth), f32),
            pltpu.VMEM((rows + 16, depth), f32),
            pltpu.VMEM((rows + 16, depth), f32),
            pltpu.SMEM(load_ratio.shape, load_ratio.dtype),
            pltpu.SemaphoreType.DMA((7,)),
            pltpu.SemaphoreType.DMA((N_SEND,)),
            pltpu.SemaphoreType.DMA((N_RECV,)),
            pltpu.SemaphoreType.REGULAR((3,)),
        ],
        compiler_params=pltpu.CompilerParams(collective_id=0, has_side_effects=True),
    )(load_ratio, density, void_mask, fixed_mask, displacement)


def solution(mesh):
    placed = (
        P(("parts", "gz"), "gy", None),
        P(("parts", "gz"), "gy", None),
        P(("parts", "gz"), "gy", None),
        P("lc", None, ("parts", "gz"), "gy", None),
        P("parts"),
    )
    return jax.shard_map(
        shards,
        mesh=mesh,
        in_specs=placed,
        out_specs=P(("parts", "gz"), "gy", None),
        check_vma=False,
    )
```

```python
import math

import jax
import jax.numpy as jnp
from jax import lax
from jax.experimental import pallas as pl
from jax.experimental.pallas import tpu as pltpu
from jax.sharding import PartitionSpec as P

MESH = pl.DeviceIdType.MESH
POISSON = 0.3
FACTOR = 1.0 / ((1.0 + POISSON) * (1.0 - 2.0 * POISSON))
LAMBDA = POISSON * FACTOR
SHEAR = (0.5 - POISSON) * FACTOR
RATIO = LAMBDA / SHEAR
W = [2.5 - math.sqrt(d) for d in range(7)]
CHUNKS = 2
EDGE = 2
N_SEND = 22
N_RECV = 31
TALL = 32
SHORT = 8


def layer_classes(q0, q1, q2, q4, q5):
    p0 = W[0] * q0 + W[1] * q1 + W[2] * q2 + W[4] * q4 + W[5] * q5
    p1 = W[1] * q0 + W[2] * q1 + W[3] * q2 + W[5] * q4 + W[6] * q5
    p2 = W[4] * q0 + W[5] * q1 + W[6] * q2
    return p0, p1, p2


def lane_index(shape):
    return lax.broadcasted_iota(jnp.int32, shape, len(shape) - 1)


def lane_pair(field, step):
    depth = field.shape[-1]
    lane = lane_index(field.shape)
    after = jnp.where(lane < depth - step, pltpu.roll(field, depth - step, 1), 0.0)
    before = jnp.where(lane >= step, pltpu.roll(field, step, 1), 0.0)
    return after + before


def cone_tiles(ref, layer, row, count):
    window = TALL + 16
    f = [ref[layer + k, pl.ds(row, window), :] for k in range(count + 4)]
    mid = slice(8, 8 + TALL)

    def pair(t, step):
        return (pltpu.roll(t, step, 0) + pltpu.roll(t, window - step, 0))[mid]

    result = []
    for k in range(count):
        x0, x1, x2 = f[k + 2], f[k + 1] + f[k + 3], f[k] + f[k + 4]
        q0 = x0[mid]
        q1 = x1[mid] + pair(x0, 1)
        q2 = pair(x1, 1)
        q4 = x2[mid] + pair(x0, 2)
        q5 = pair(x2, 1) + pair(x1, 2)
        p0, p1, p2 = layer_classes(q0, q1, q2, q4, q5)
        result.append(p0 + lane_pair(p1, 1) + lane_pair(p2, 2))
    return result


def boundary_cones(ref, layer, row, reaches):
    window = TALL + 16
    t = ref[layer, pl.ds(row, window), :]
    mid = slice(8, 8 + TALL)
    t0 = t[mid]
    t1, t2 = [
        (pltpu.roll(t, step, 0) + pltpu.roll(t, window - step, 0))[mid] for step in (1, 2)
    ]
    result = []
    for reach in reaches:
        if reach == 0:
            p0 = W[0] * t0 + W[1] * t1 + W[4] * t2
            p1 = W[1] * t0 + W[2] * t1 + W[5] * t2
            p2 = W[4] * t0 + W[5] * t1
        elif reach == 1:
            p0 = W[1] * t0 + W[2] * t1 + W[5] * t2
            p1 = W[2] * t0 + W[3] * t1 + W[6] * t2
            p2 = W[5] * t0 + W[6] * t1
        else:
            p0, p1, p2 = W[4] * t0 + W[5] * t1, W[5] * t0 + W[6] * t1, None
        total = p0 + lane_pair(p1, 1)
        result.append(total if p2 is None else total + lane_pair(p2, 2))
    return result


def present(position, total, step):
    before = (position >= step).astype(jnp.float32)
    return before + (position + step < total).astype(jnp.float32)


def weight_tile(layer, layers, row, rows, depth):
    shape = (TALL, depth)
    sub = lax.broadcasted_iota(jnp.int32, shape, 0) + row
    spot = jnp.full(shape, layer, jnp.int32)
    nx1, nx2 = present(spot, layers, 1), present(spot, layers, 2)
    ny1, ny2 = present(sub, rows, 1), present(sub, rows, 2)
    one = jnp.ones(shape, jnp.float32)
    p0, p1, p2 = layer_classes(one, nx1 + ny1, nx1 * ny1, nx2 + ny2, nx2 * ny1 + nx1 * ny2)
    lane = lane_index(shape)
    return p0 + present(lane, depth, 1) * p1 + present(lane, depth, 2) * p2


def node_modes(ref, layer, row):
    result = []
    for comp in range(3):
        t = ref[comp, layer, pl.ds(row, SHORT + 8), :]
        depth, window = t.shape[-1], t.shape[0]
        here, after = t[0:SHORT], pltpu.roll(t, window - 1, 0)[0:SHORT]
        s, d = here + after, after - here
        inner = lane_index(s.shape) < depth - 1
        sn = jnp.where(inner, pltpu.roll(s, depth - 1, 1), 0.0)
        dn = jnp.where(inner, pltpu.roll(d, depth - 1, 1), 0.0)
        result.append((s + sn, sn - s, d + dn, dn - d))
    return result


def energy_tile(lower, upper):
    modes = []
    for a, b in zip(lower, upper):
        modes.append(
            {
                "x": b[0] - a[0],
                "z": a[1] + b[1],
                "y": a[2] + b[2],
                "yz": a[3] + b[3],
                "xz": b[1] - a[1],
                "xy": b[2] - a[2],
                "xyz": b[3] - a[3],
            }
        )
    u, v, w = modes
    sq = lambda t: t * t
    trace = sq(u["x"] + v["y"] + w["z"])
    normal = sq(u["x"]) + sq(v["y"]) + sq(w["z"])
    bend = sq(u["xy"]) + sq(u["xz"]) + sq(v["xy"]) + sq(v["yz"]) + sq(w["yz"]) + sq(w["xz"])
    cross = v["xy"] * w["xz"] + u["xy"] * w["yz"] + u["xz"] * v["yz"]
    shear = sq(u["y"] + v["x"]) + sq(u["z"] + w["x"]) + sq(v["z"] + w["y"])
    pair = v["xz"] + w["xy"]
    twist = u["yz"] * (u["yz"] + pair) + v["xz"] * pair + sq(w["xy"])
    cubic = sq(u["xyz"]) + sq(v["xyz"]) + sq(w["xyz"])
    return (
        RATIO * trace
        + 2.0 * normal
        + (1.0 + RATIO / 3.0) * bend
        + (2.0 * RATIO / 3.0) * cross
        + shear
        + (2.0 / 3.0) * twist
        + ((RATIO + 4.0) / 9.0) * cubic
    )


def kernel(
    ratio_in, density, void, fixed, disp, out,
    moved, fix, col_s, col_r, cor_s, cor_r, dens, dead, scale, energy, other, sens, mine, peer, hold, ratio,
    border, rim, held, local, send, recv, ready,
):
    layers, rows, depth = density.shape
    half = layers // 2
    r, c, h = lax.axis_index("gz"), lax.axis_index("gy"), lax.axis_index("lc")
    nr, nc = lax.axis_size("gz"), lax.axis_size("gy")
    dz = 1 - 2 * h
    mid = pl.ds(8, rows)
    low, high = pl.ds(0, 8), pl.ds(rows + 8, 8)

    def there(step_z, step_y):
        z, y = r + step_z, c + step_y
        return (z >= 0) & (z < nr) & (y >= 0) & (y < nc)

    def remote(index, src, dst, step_z, step_y, core, slot=None):
        copy = pltpu.make_async_remote_copy(
            src_ref=src, dst_ref=dst, send_sem=send.at[index if slot is None else slot],
            recv_sem=recv.at[index],
            device_id={"gz": r + step_z, "gy": c + step_y, "lc": core}, device_id_type=MESH,
        )
        goes, comes = there(step_z, step_y), there(-step_z, -step_y)
        return copy, goes, comes

    def between(index, src, dst, giver, slot=None):
        taker = 1 - giver
        copy, goes, comes = remote(index, src, dst, 0, 0, taker, slot)
        return copy, goes & (h == giver), comes & (h == taker)

    def flipped(index, src, dst, step_y, slot=None):
        copy, goes, _ = remote(index, src, dst, -dz, step_y, 1 - h, slot)
        return copy, goes, there(-dz, -step_y)

    def start(entry, when=True):
        copy, goes, _ = entry
        pl.when(goes & when)(copy.start)

    def arrive(entry):
        copy, _, comes = entry
        pl.when(comes)(copy.wait_recv)

    def left(entry):
        copy, goes, _ = entry
        pl.when(goes)(copy.wait_send)

    l0, b0 = half // 2 * (1 - h), half // 2 * h
    keep = half + 2
    lz, sb = (half + 2) * h, (layers - 2) * (1 - h)
    plane = pl.ds(0, rows)
    given, halo = (layers - 1) * (1 - h), (layers + 1) * h
    get_disp = pltpu.make_async_copy(
        disp.at[0], moved.at[:, pl.ds(1, layers), plane, :], local.at[0]
    )
    get_fix = pltpu.make_async_copy(fixed, fix, local.at[1])
    get_rim = pltpu.make_async_copy(disp.at[0, :, :, pl.ds(0, 1), :], rim, local.at[6])
    get_held = pltpu.make_async_copy(fixed.at[:, pl.ds(0, 1), :], held, local.at[7])
    get_dens = pltpu.make_async_copy(
        density.at[pl.ds(b0, keep)], dens.at[pl.ds(l0, keep), mid, :], local.at[2]
    )
    get_dead = pltpu.make_async_copy(void.at[pl.ds(half * h, half)], dead, local.at[3])
    get_ratio = pltpu.make_async_copy(ratio_in, ratio, local.at[4])
    get_border = pltpu.make_async_copy(density.at[pl.ds(sb, 2)], border, local.at[5])
    for copy in (get_rim, get_held, get_border, get_dens, get_disp, get_fix, get_ratio, get_dead):
        copy.start()

    barrier = pltpu.get_barrier_semaphore()
    def greet(semaphore, step_z, step_y, core):
        @pl.when(there(step_z, step_y))
        def _():
            pl.semaphore_signal(
                semaphore, inc=1,
                device_id={"gz": r + step_z, "gy": c + step_y, "lc": core},
                device_id_type=MESH,
            )

    flag = lambda value: value.astype(jnp.int32)

    def await_from(semaphore, step_z, step_y, count):
        @pl.when(there(step_z, step_y))
        def _():
            pl.semaphore_wait(semaphore, count)

    for core in (h, 1 - h):
        greet(barrier, 1, 0, core)
        greet(barrier, 0, 1, core)
    greet(barrier, 0, 0, 1 - h)

    near, far = pl.ds(l0, keep), pl.ds(lz, 2)
    tiles = rows // SHORT
    head = (tiles - 2) * SHORT
    swap_rows = [pl.ds(0, head), pl.ds(head, rows - head)]
    top, bottom = pl.ds(rows - EDGE, EDGE), pl.ds(0, EDGE)
    above, below = pl.ds(8 - EDGE, EDGE), pl.ds(rows + 8, EDGE)
    last, first = pl.ds(rows + 8 - EDGE, EDGE), pl.ds(8, EDGE)
    dens_rows = [
        remote(1, dens.at[near, last, :], dens.at[near, above, :], 0, 1, h),
        remote(2, dens.at[near, first, :], dens.at[near, below, :], 0, -1, h),
    ]
    dens_far = [
        remote(0, border.at[:, swap_rows[0], :], dens.at[far, pl.ds(8, head), :], dz, 0, h),
        remote(3, border.at[:, top, :], dens.at[far, above, :], dz, 1, h),
        remote(4, border.at[:, bottom, :], dens.at[far, below, :], dz, -1, h),
        remote(30, border.at[:, swap_rows[1], :], dens.at[far, pl.ds(8 + head, rows - head), :], dz, 0, h, 21),
    ]

    def free_layer(i):
        free = (1 - fix[i]).astype(jnp.float32)
        for comp in range(3):
            moved[comp, i + 1, plane, :] = moved[comp, i + 1, plane, :] * free

    tall = rows // CHUNKS
    parts = [pl.ds(q * tall, tall) for q in range(CHUNKS)]
    send_disp = [
        remote(5 + q, moved.at[:, given + 1, part, :], moved.at[:, halo, part, :], dz, 0, h)
        for q, part in enumerate(parts)
    ]
    send_col = remote(7, col_s, col_r, 0, -1, h)
    send_cor = remote(8, cor_s, cor_r, dz, -1, h)
    pl.semaphore_wait(barrier, 2 * (flag(r > 0) + flag(c > 0)) + 1)
    for core in (h, 1 - h):
        greet(ready.at[0], -1, 0, core)
        greet(ready.at[1], 0, -1, core)
    get_rim.wait()
    get_held.wait()
    for i in range(layers):
        free = (1 - held[i]).astype(jnp.float32)
        for comp in range(3):
            col_s[comp, i : i + 1, :] = rim[comp, i] * free
    start(send_col)
    for comp in range(3):
        cor_s[comp : comp + 1, :] = rim[comp, given] * (1 - held[given]).astype(jnp.float32)
    get_border.wait()
    start(dens_far[0], h == 1)
    get_dens.wait()
    start(dens_rows[1])
    get_disp.wait()
    get_fix.wait()

    def free_step(i, _):
        free_layer(i)
        return 0

    lax.fori_loop(0, layers, free_step, 0)
    await_from(ready.at[0], 1, 0, 2)
    start(dens_far[0], h == 0)
    await_from(ready.at[1], 0, 1, 2)
    start(dens_rows[0])
    greet(ready.at[3], 0, -1, h)
    greet(ready.at[2], 0, 1, h)

    get_ratio.wait()
    ratio_sum = ratio[0]
    for case in range(1, ratio.shape[0]):
        ratio_sum = ratio_sum + ratio[case]
    total = jnp.full((8, depth), ratio_sum.astype(jnp.float32))
    share = (SHEAR / 16.0) * (jnp.full((8, depth), ratio[h].astype(jnp.float32)) / total)


    def energy_rows(first, count, j):
        row = pl.multiple_of(j * SHORT, SHORT)
        lower = node_modes(moved, first + 1, row)
        for k in range(count):
            upper = node_modes(moved, first + k + 2, row)
            energy[first + k, pl.ds(row, SHORT), :] = share * energy_tile(lower, upper)
            lower = upper

    def energy_layers(first, count, begin, end):
        def tile(j, _):
            energy_rows(first, count, begin + 2 * j)
            energy_rows(first, count, begin + 2 * j + 1)
            return 0

        lax.fori_loop(0, (end - begin) // 2, tile, 0)

    close, wide = 2 * (1 - h), 2 * h

    def scale_rows(j, row):
        cones = cone_tiles(dens, j, row, 2)
        for n in range(2):
            weights = weight_tile(
                r * layers + half * h + j + n, nr * layers, c * rows + row, nc * rows, depth
            )
            inverse = 1.0 / weights
            physical = cones[n] * inverse
            alive = (1 - dead[j + n, pl.ds(row, TALL), :]).astype(jnp.float32)
            scale[j + n, pl.ds(row, TALL), :] = (
                alive * (-3.0 * (1.0 - 0.001)) * physical * physical * inverse
            )

    def scale_two(j):
        def tile(k, _):
            scale_rows(j, pl.multiple_of(k * TALL, TALL))
            return 0

        lax.fori_loop(0, rows // TALL, tile, 0)

    give = half * (1 - h)
    swap_a = [
        remote(
            9 + q, energy.at[pl.ds(give, half - 1), part, :],
            other.at[pl.ds(0, half - 1), part, :], 0, 0, 1 - h,
        )
        for q, part in enumerate(swap_rows)
    ]
    swap_b = [
        between(11 + q, energy.at[half - 1, part, :], other.at[half - 1, part, :], 1)
        for q, part in enumerate(swap_rows)
    ]
    rest = (half - 1) * h
    energy_layers(give, half - 1, 0, tiles - 2)
    start(swap_a[0])
    await_from(ready.at[2], 0, -1, 1)
    for entry in [dens_far[2], send_cor, dens_far[3], send_disp[1]]:
        start(entry)
    energy_layers(rest, half, 0, tiles - 2)
    start(swap_b[0])
    await_from(ready.at[3], 0, 1, 1)
    for entry in [dens_far[1], send_disp[0]]:
        start(entry)

    blank = jnp.zeros((8, depth), jnp.float32)

    @pl.when(r == nr - 1)
    def _():
        for comp in range(3):
            moved[comp, layers + 1, plane, :] = jnp.zeros((rows, depth), jnp.float32)
            moved[comp, layers + 1, pl.ds(rows, 8), :] = blank

    @pl.when(c == nc - 1)
    def _():
        col_r[...] = jnp.zeros_like(col_r)

    @pl.when(jnp.logical_not(there(-dz, 1)))
    def _():
        cor_r[...] = jnp.zeros_like(cor_r)

    @pl.when(c == 0)
    def _():
        mine[low, :] = blank
        peer[low, :] = blank

    @pl.when(c == nc - 1)
    def _():
        mine[high, :] = blank
        peer[high, :] = blank

    for ref in (dens, sens):

        @pl.when(c == 0)
        def _():
            for i in range(half + 4):
                ref[i, low, :] = blank

        @pl.when(c == nc - 1)
        def _():
            for i in range(half + 4):
                ref[i, high, :] = blank

        @pl.when(jnp.logical_not(there(-dz, 0)))
        def _():
            for i in range(2):
                ref[lz + i] = jnp.zeros((rows + 16, depth), jnp.float32)

    get_dead.wait()
    for entry in dens_rows:
        arrive(entry)
    scale_two(close)
    arrive(send_col)
    for comp in range(3):
        for i in range(layers):
            moved[comp, i + 1, pl.ds(rows, 1), :] = col_r[comp, i : i + 1, :]
    energy_layers(give, half - 1, tiles - 2, tiles)
    start(swap_a[1])
    energy_layers(rest, half, tiles - 2, tiles)
    start(swap_b[1])

    def sense(j):
        sens[2 + j, mid, :] = scale[j] * (energy[half * h + j] + other[j])

    strip_count = rows // TALL
    arrive(dens_far[0])
    arrive(dens_far[3])
    for k in range(strip_count):
        strip = (k + strip_count - c % strip_count) % strip_count
        for entry, at in ((dens_far[1], 0), (dens_far[2], strip_count - 1)):
            copy, goes, comes = entry
            arrive((copy, goes, comes & (strip == at)))
        scale_rows(wide, pl.multiple_of(strip * TALL, TALL))
    for entry in swap_a + swap_b:
        arrive(entry)

    ps, pd = pl.ds(half - (half - 2) * h, 2), pl.ds((half + 2) * h, 2)
    zs, zd = pl.ds(2 + (half - 2) * h, 2), pl.ds((half + 2) * (1 - h), 2)
    close_copies = [
        remote(13, sens.at[ps, mid, :], sens.at[pd, mid, :], 0, 0, 1 - h),
        remote(16, sens.at[ps, last, :], sens.at[pd, above, :], 0, 1, 1 - h),
        remote(17, sens.at[ps, first, :], sens.at[pd, below, :], 0, -1, 1 - h),
    ]
    wide_copies = [
        flipped(18, sens.at[zs, last, :], sens.at[zd, above, :], 1),
        flipped(19, sens.at[zs, first, :], sens.at[zd, below, :], -1),
        flipped(20, sens.at[zs, mid, :], sens.at[zd, mid, :], 0),
    ]
    core_rows = pl.ds(2, half)
    row_copies = [
        remote(14, sens.at[core_rows, last, :], sens.at[core_rows, above, :], 0, 1, h),
        remote(15, sens.at[core_rows, first, :], sens.at[core_rows, below, :], 0, -1, h),
    ]
    edge_copies = [
        remote(21, mine.at[last, :], mine.at[above, :], 0, 1, h, 0),
        remote(22, mine.at[first, :], mine.at[below, :], 0, -1, h, 1),
        flipped(23, mine.at[last, :], peer.at[above, :], 1, 2),
        flipped(24, mine.at[first, :], peer.at[below, :], -1, 3),
    ]
    main_copies = [
        flipped(25 + q, mine.at[pl.ds(8 + q * tall, tall), :], peer.at[pl.ds(8 + q * tall, tall), :], 0, 4 + q)
        for q in range(CHUNKS)
    ]
    atop = (r == nr - 1) & (h == 0)
    whole = energy.at[layers - 1]
    top_copies = [
        remote(23, whole.at[top, :], peer.at[above, :], 0, 1, 1, 6),
        remote(24, whole.at[bottom, :], peer.at[below, :], 0, -1, 1, 7),
        remote(25, whole.at[parts[0], :], peer.at[pl.ds(8, tall), :], 0, 0, 1, 8),
        remote(26, whole.at[parts[1], :], peer.at[pl.ds(8 + tall, tall), :], 0, 0, 1, 9),
    ]
    top_copies = [
        (copy, goes & atop, comes & (r == nr - 1) & (h == 1)) for copy, goes, comes in top_copies
    ]
    joined = (h == 1) | (r > 0)
    edge_copies[:2] = [(copy, goes & joined, comes & joined) for copy, goes, comes in edge_copies[:2]]
    arrivals = [
        (copy, goes, comes | extra)
        for (copy, goes, comes), (_, _, extra) in zip(edge_copies[2:] + main_copies, top_copies)
    ]
    pieces = [
        [edge_copies[1], edge_copies[3], main_copies[0]],
        [edge_copies[0], edge_copies[2], main_copies[1]],
    ]

    def boundary():
        for entry in [*dens_rows, *dens_far, *send_disp, send_col, send_cor, *swap_a, *swap_b]:
            left(entry)

        @pl.when(atop)
        def _():
            energy_layers(layers - 1, 1, 0, tiles)

        for entry in top_copies:
            start(entry)
        arrive(send_cor)
        for comp in range(3):
            moved[comp, halo, pl.ds(rows, 1), :] = cor_r[comp : comp + 1, :]
        for q in reversed(range(CHUNKS)):
            arrive(send_disp[q])

            @pl.when(joined)
            def _():
                for n in range(tall // SHORT):
                    row = q * tall + n * SHORT
                    mine[pl.ds(row + 8, SHORT), :] = share * energy_tile(
                        node_modes(moved, layers * h, row), node_modes(moved, layers * h + 1, row)
                    )

            for entry in pieces[q]:
                start(entry)

    def spread():
        sense(wide)

        @pl.when(h == 0)
        def _():
            sense(1)

        @pl.when(h == 1)
        def _():
            sens[half + 1, mid, :] = scale[half - 1]

        for entry in wide_copies:
            start(entry)
        sense(close)
        sense(close + 1)
        for entry in close_copies + row_copies:
            start(entry)

    spread()
    boundary()

    def filter_rows(j, count, row):
        cones = cone_tiles(sens, j, row, count)
        for n in range(count):
            alive = (1 - dead[j + n, pl.ds(row, TALL), :]).astype(jnp.float32)
            out[half * h + j + n, pl.ds(row, TALL), :] = alive * cones[n]

    def filter_layers(j, count):
        def tile(k, _):
            filter_rows(j, count, pl.multiple_of(k * TALL, TALL))
            return 0

        lax.fori_loop(0, rows // TALL, tile, 0)

    def hand_over(index, giver, j, count, part):
        place = out.at[pl.ds(half * giver + j, count), part, :]
        return between(index, place, place, giver, index - 17)

    early = [hand_over(27, 0, 2, half - 2, plane), hand_over(27, 1, 0, half - 3, plane)]
    strips = [pl.ds(k * TALL, TALL) for k in range(rows // TALL)]
    late = [
        [hand_over(28 + k, 0, 0, 2, strip), hand_over(28 + k, 1, half - 3, 3, strip)]
        for k, strip in enumerate(strips)
    ]
    for entry in close_copies + row_copies:
        arrive(entry)

    @pl.when(h == 0)
    def _():
        filter_layers(2, half - 2)

    @pl.when(h == 1)
    def _():
        filter_layers(0, half - 3)

    for entry in early:
        start(entry)
    for entry in close_copies + row_copies:
        left(entry)
    for entry in wide_copies:
        arrive(entry)
    for entry in wide_copies:
        left(entry)
    for entry in edge_copies + main_copies + top_copies:
        left(entry)
    b = 1 + half * h

    @pl.when(joined)
    def _():
        hold[...] = sens[b]
        sens[b] = jnp.zeros((rows + 16, depth), jnp.float32)

    def partial_layers(j, count):
        def tile(k, _):
            row = pl.multiple_of(k * TALL, TALL)
            for n, cone in enumerate(cone_tiles(sens, j, row, count)):
                out[half * h + j + n, pl.ds(row, TALL), :] = cone
            return 0

        lax.fori_loop(0, rows // TALL, tile, 0)

    @pl.when(h == 0)
    def _():
        partial_layers(0, 2)

    @pl.when(h == 1)
    def _():
        partial_layers(half - 3, 3)

    def finish_rows(pairs, row):
        for (j, reach), cone in zip(pairs, boundary_cones(sens, b, row, [p[1] for p in pairs])):
            alive = (1 - dead[j, pl.ds(row, TALL), :]).astype(jnp.float32)
            here = pl.ds(row, TALL)
            out[half * h + j, here, :] = alive * (out[half * h + j, here, :] + cone)

    for entry in edge_copies[:2] + arrivals:
        arrive(entry)

    @pl.when(joined)
    def _():
        sens[b] = hold[...] * (mine[...] + peer[...])

    for k in range(rows // TALL):

        @pl.when(h == 0)
        def _():
            finish_rows([(0, 1), (1, 2)], k * TALL)

        @pl.when(h == 1)
        def _():
            finish_rows([(half - 3, 2), (half - 2, 1), (half - 1, 0)], k * TALL)

        for entry in late[k]:
            start(entry)
    late = [entry for pair in late for entry in pair]
    for entry in early + late:
        left(entry)
    for entry in early + late:
        arrive(entry)


def shards(density, void_mask, fixed_mask, displacement, load_ratio):
    layers, rows, depth = density.shape
    half = layers // 2
    f32 = jnp.float32
    hbm = pl.BlockSpec(memory_space=pl.ANY)
    return pl.pallas_call(
        kernel,
        out_shape=pltpu.VMEM(density.shape, f32),
        in_specs=[hbm] * 5,
        out_specs=pl.BlockSpec(memory_space=pltpu.VMEM),
        scratch_shapes=[
            pltpu.VMEM((3, layers + 2, rows + 8, depth), f32),
            pltpu.VMEM((layers, rows, depth), jnp.int32),
            pltpu.VMEM((3, layers, depth), f32),
            pltpu.VMEM((3, layers, depth), f32),
            pltpu.VMEM((8, depth), f32),
            pltpu.VMEM((8, depth), f32),
            pltpu.VMEM((half + 4, rows + 16, depth), f32),
            pltpu.VMEM((half, rows, depth), jnp.int32),
            pltpu.VMEM((half, rows, depth), f32),
            pltpu.VMEM((layers, rows, depth), f32),
            pltpu.VMEM((half, rows, depth), f32),
            pltpu.VMEM((half + 4, rows + 16, depth), f32),
            pltpu.VMEM((rows + 16, depth), f32),
            pltpu.VMEM((rows + 16, depth), f32),
            pltpu.VMEM((rows + 16, depth), f32),
            pltpu.SMEM(load_ratio.shape, load_ratio.dtype),
            pltpu.VMEM((2, rows, depth), f32),
            pltpu.VMEM((3, layers, 1, depth), f32),
            pltpu.VMEM((layers, 1, depth), jnp.int32),
            pltpu.SemaphoreType.DMA((8,)),
            pltpu.SemaphoreType.DMA((N_SEND,)),
            pltpu.SemaphoreType.DMA((N_RECV,)),
            pltpu.SemaphoreType.REGULAR((4,)),
        ],
        compiler_params=pltpu.CompilerParams(collective_id=0, has_side_effects=True),
    )(load_ratio, density, void_mask, fixed_mask, displacement)


def solution(mesh):
    placed = (
        P(("parts", "gz"), "gy", None),
        P(("parts", "gz"), "gy", None),
        P(("parts", "gz"), "gy", None),
        P("lc", None, ("parts", "gz"), "gy", None),
        P("parts"),
    )
    return jax.shard_map(
        shards,
        mesh=mesh,
        in_specs=placed,
        out_specs=P(("parts", "gz"), "gy", None),
        check_vma=False,
    )
```

```python
import math

import jax
import jax.numpy as jnp
from jax import lax
from jax.experimental import pallas as pl
from jax.experimental.pallas import tpu as pltpu
from jax.sharding import PartitionSpec as P

MESH = pl.DeviceIdType.MESH
POISSON = 0.3
FACTOR = 1.0 / ((1.0 + POISSON) * (1.0 - 2.0 * POISSON))
LAMBDA = POISSON * FACTOR
SHEAR = (0.5 - POISSON) * FACTOR
RATIO = LAMBDA / SHEAR
W = [2.5 - math.sqrt(d) for d in range(7)]
CHUNKS = 2
EDGE = 2
N_SEND = 23
N_RECV = 32
TALL = 32
SHORT = 8


def layer_classes(q0, q1, q2, q4, q5):
    p0 = W[0] * q0 + W[1] * q1 + W[2] * q2 + W[4] * q4 + W[5] * q5
    p1 = W[1] * q0 + W[2] * q1 + W[3] * q2 + W[5] * q4 + W[6] * q5
    p2 = W[4] * q0 + W[5] * q1 + W[6] * q2
    return p0, p1, p2


def lane_index(shape):
    return lax.broadcasted_iota(jnp.int32, shape, len(shape) - 1)


def lane_pair(field, step):
    depth = field.shape[-1]
    lane = lane_index(field.shape)
    after = jnp.where(lane < depth - step, pltpu.roll(field, depth - step, 1), 0.0)
    before = jnp.where(lane >= step, pltpu.roll(field, step, 1), 0.0)
    return after + before


def cone_tiles(ref, layer, row, count):
    window = TALL + 16
    f = [ref[layer + k, pl.ds(row, window), :] for k in range(count + 4)]
    mid = slice(8, 8 + TALL)

    def pair(t, step):
        return (pltpu.roll(t, step, 0) + pltpu.roll(t, window - step, 0))[mid]

    result = []
    for k in range(count):
        x0, x1, x2 = f[k + 2], f[k + 1] + f[k + 3], f[k] + f[k + 4]
        q0 = x0[mid]
        q1 = x1[mid] + pair(x0, 1)
        q2 = pair(x1, 1)
        q4 = x2[mid] + pair(x0, 2)
        q5 = pair(x2, 1) + pair(x1, 2)
        p0, p1, p2 = layer_classes(q0, q1, q2, q4, q5)
        result.append(p0 + lane_pair(p1, 1) + lane_pair(p2, 2))
    return result


def boundary_cones(ref, layer, row, reaches):
    window = TALL + 16
    t = ref[layer, pl.ds(row, window), :]
    mid = slice(8, 8 + TALL)
    t0 = t[mid]
    t1, t2 = [
        (pltpu.roll(t, step, 0) + pltpu.roll(t, window - step, 0))[mid] for step in (1, 2)
    ]
    result = []
    for reach in reaches:
        if reach == 0:
            p0 = W[0] * t0 + W[1] * t1 + W[4] * t2
            p1 = W[1] * t0 + W[2] * t1 + W[5] * t2
            p2 = W[4] * t0 + W[5] * t1
        elif reach == 1:
            p0 = W[1] * t0 + W[2] * t1 + W[5] * t2
            p1 = W[2] * t0 + W[3] * t1 + W[6] * t2
            p2 = W[5] * t0 + W[6] * t1
        else:
            p0, p1, p2 = W[4] * t0 + W[5] * t1, W[5] * t0 + W[6] * t1, None
        total = p0 + lane_pair(p1, 1)
        result.append(total if p2 is None else total + lane_pair(p2, 2))
    return result


def present(position, total, step):
    before = (position >= step).astype(jnp.float32)
    return before + (position + step < total).astype(jnp.float32)


def weight_tile(layer, layers, row, rows, depth):
    shape = (TALL, depth)
    sub = lax.broadcasted_iota(jnp.int32, shape, 0) + row
    spot = jnp.full(shape, layer, jnp.int32)
    nx1, nx2 = present(spot, layers, 1), present(spot, layers, 2)
    ny1, ny2 = present(sub, rows, 1), present(sub, rows, 2)
    one = jnp.ones(shape, jnp.float32)
    p0, p1, p2 = layer_classes(one, nx1 + ny1, nx1 * ny1, nx2 + ny2, nx2 * ny1 + nx1 * ny2)
    lane = lane_index(shape)
    return p0 + present(lane, depth, 1) * p1 + present(lane, depth, 2) * p2


def node_modes(ref, layer, row):
    result = []
    for comp in range(3):
        t = ref[comp, layer, pl.ds(row, SHORT + 8), :]
        depth, window = t.shape[-1], t.shape[0]
        here, after = t[0:SHORT], pltpu.roll(t, window - 1, 0)[0:SHORT]
        s, d = here + after, after - here
        inner = lane_index(s.shape) < depth - 1
        sn = jnp.where(inner, pltpu.roll(s, depth - 1, 1), 0.0)
        dn = jnp.where(inner, pltpu.roll(d, depth - 1, 1), 0.0)
        result.append((s + sn, sn - s, d + dn, dn - d))
    return result


def energy_tile(lower, upper):
    modes = []
    for a, b in zip(lower, upper):
        modes.append(
            {
                "x": b[0] - a[0],
                "z": a[1] + b[1],
                "y": a[2] + b[2],
                "yz": a[3] + b[3],
                "xz": b[1] - a[1],
                "xy": b[2] - a[2],
                "xyz": b[3] - a[3],
            }
        )
    u, v, w = modes
    sq = lambda t: t * t
    trace = sq(u["x"] + v["y"] + w["z"])
    normal = sq(u["x"]) + sq(v["y"]) + sq(w["z"])
    bend = sq(u["xy"]) + sq(u["xz"]) + sq(v["xy"]) + sq(v["yz"]) + sq(w["yz"]) + sq(w["xz"])
    cross = v["xy"] * w["xz"] + u["xy"] * w["yz"] + u["xz"] * v["yz"]
    shear = sq(u["y"] + v["x"]) + sq(u["z"] + w["x"]) + sq(v["z"] + w["y"])
    pair = v["xz"] + w["xy"]
    twist = u["yz"] * (u["yz"] + pair) + v["xz"] * pair + sq(w["xy"])
    cubic = sq(u["xyz"]) + sq(v["xyz"]) + sq(w["xyz"])
    return (
        RATIO * trace
        + 2.0 * normal
        + (1.0 + RATIO / 3.0) * bend
        + (2.0 * RATIO / 3.0) * cross
        + shear
        + (2.0 / 3.0) * twist
        + ((RATIO + 4.0) / 9.0) * cubic
    )


def kernel(
    ratio_in, density, void, fixed, disp, out,
    moved, fix, col_s, col_r, cor_s, cor_r, dens, dead, scale, energy, other, sens, mine, peer, hold, ratio,
    border, rim, held, local, send, recv, ready,
):
    layers, rows, depth = density.shape
    half = layers // 2
    r, c, h = lax.axis_index("gz"), lax.axis_index("gy"), lax.axis_index("lc")
    nr, nc = lax.axis_size("gz"), lax.axis_size("gy")
    dz = 1 - 2 * h
    mid = pl.ds(8, rows)
    low, high = pl.ds(0, 8), pl.ds(rows + 8, 8)

    def there(step_z, step_y):
        z, y = r + step_z, c + step_y
        return (z >= 0) & (z < nr) & (y >= 0) & (y < nc)

    def remote(index, src, dst, step_z, step_y, core, slot=None):
        copy = pltpu.make_async_remote_copy(
            src_ref=src, dst_ref=dst, send_sem=send.at[index if slot is None else slot],
            recv_sem=recv.at[index],
            device_id={"gz": r + step_z, "gy": c + step_y, "lc": core}, device_id_type=MESH,
        )
        goes, comes = there(step_z, step_y), there(-step_z, -step_y)
        return copy, goes, comes

    def between(index, src, dst, giver, slot=None):
        taker = 1 - giver
        copy, goes, comes = remote(index, src, dst, 0, 0, taker, slot)
        return copy, goes & (h == giver), comes & (h == taker)

    def flipped(index, src, dst, step_y, slot=None):
        copy, goes, _ = remote(index, src, dst, -dz, step_y, 1 - h, slot)
        return copy, goes, there(-dz, -step_y)

    def start(entry, when=True):
        copy, goes, _ = entry
        pl.when(goes & when)(copy.start)

    def arrive(entry):
        copy, _, comes = entry
        pl.when(comes)(copy.wait_recv)

    def left(entry):
        copy, goes, _ = entry
        pl.when(goes)(copy.wait_send)

    l0, b0 = half // 2 * (1 - h), half // 2 * h
    keep = half + 2
    lz, sb = (half + 2) * h, (layers - 2) * (1 - h)
    plane = pl.ds(0, rows)
    given, halo = (layers - 1) * (1 - h), (layers + 1) * h
    get_disp = pltpu.make_async_copy(
        disp.at[0], moved.at[:, pl.ds(1, layers), plane, :], local.at[0]
    )
    get_fix = pltpu.make_async_copy(fixed, fix, local.at[1])
    get_rim = pltpu.make_async_copy(disp.at[0, :, :, pl.ds(0, 1), :], rim, local.at[6])
    get_held = pltpu.make_async_copy(fixed.at[:, pl.ds(0, 1), :], held, local.at[7])
    get_dens = pltpu.make_async_copy(
        density.at[pl.ds(b0, keep)], dens.at[pl.ds(l0, keep), mid, :], local.at[2]
    )
    get_dead = pltpu.make_async_copy(void.at[pl.ds(half * h, half)], dead, local.at[3])
    get_ratio = pltpu.make_async_copy(ratio_in, ratio, local.at[4])
    get_border = pltpu.make_async_copy(density.at[pl.ds(sb, 2)], border, local.at[5])
    for copy in (get_rim, get_held, get_border, get_dens, get_disp, get_fix, get_ratio, get_dead):
        copy.start()

    barrier = pltpu.get_barrier_semaphore()
    def greet(semaphore, step_z, step_y, core):
        @pl.when(there(step_z, step_y))
        def _():
            pl.semaphore_signal(
                semaphore, inc=1,
                device_id={"gz": r + step_z, "gy": c + step_y, "lc": core},
                device_id_type=MESH,
            )

    flag = lambda value: value.astype(jnp.int32)

    def await_from(semaphore, step_z, step_y, count):
        @pl.when(there(step_z, step_y))
        def _():
            pl.semaphore_wait(semaphore, count)

    for core in (h, 1 - h):
        greet(barrier, 1, 0, core)
        greet(barrier, 0, 1, core)
    greet(barrier, 0, 0, 1 - h)

    near, far = pl.ds(l0, keep), pl.ds(lz, 2)
    tiles = rows // SHORT
    head = (tiles - 2) * SHORT
    swap_rows = [pl.ds(0, head), pl.ds(head, rows - head)]
    top, bottom = pl.ds(rows - EDGE, EDGE), pl.ds(0, EDGE)
    above, below = pl.ds(8 - EDGE, EDGE), pl.ds(rows + 8, EDGE)
    last, first = pl.ds(rows + 8 - EDGE, EDGE), pl.ds(8, EDGE)
    dens_rows = [
        remote(1, dens.at[near, last, :], dens.at[near, above, :], 0, 1, h),
        remote(2, dens.at[near, first, :], dens.at[near, below, :], 0, -1, h),
    ]
    dens_far = [
        remote(0, border.at[:, swap_rows[0], :], dens.at[far, pl.ds(8, head), :], dz, 0, h),
        remote(3, border.at[:, top, :], dens.at[far, above, :], dz, 1, h),
        remote(4, border.at[:, bottom, :], dens.at[far, below, :], dz, -1, h),
        remote(30, border.at[:, swap_rows[1], :], dens.at[far, pl.ds(8 + head, rows - head), :], dz, 0, h, 21),
    ]

    def free_layer(i):
        free = (1 - fix[i]).astype(jnp.float32)
        for comp in range(3):
            moved[comp, i + 1, plane, :] = moved[comp, i + 1, plane, :] * free

    tall = rows // CHUNKS
    parts = [pl.ds(0, tall + SHORT), pl.ds(tall + SHORT, rows - tall - SHORT)]
    halves = [pl.ds(q * tall, tall) for q in range(CHUNKS)]
    send_disp = [
        remote(5 + q, moved.at[:, given + 1, part, :], moved.at[:, halo, part, :], dz, 0, h)
        for q, part in enumerate(parts)
    ]
    send_col = remote(7, col_s, col_r, 0, -1, h)
    send_cor = remote(8, cor_s, cor_r, dz, -1, h)
    pl.semaphore_wait(barrier, 2 * (flag(r > 0) + flag(c > 0)) + 1)
    for core in (h, 1 - h):
        greet(ready.at[0], -1, 0, core)
        greet(ready.at[1], 0, -1, core)
    get_rim.wait()
    get_held.wait()
    for i in range(layers):
        free = (1 - held[i]).astype(jnp.float32)
        for comp in range(3):
            col_s[comp, i : i + 1, :] = rim[comp, i] * free
    start(send_col)
    for comp in range(3):
        cor_s[comp : comp + 1, :] = rim[comp, given] * (1 - held[given]).astype(jnp.float32)
    get_border.wait()
    start(dens_far[0], h == 1)
    get_dens.wait()
    start(dens_rows[1])
    get_disp.wait()
    await_from(ready.at[0], 1, 0, 2)
    start(dens_far[0], h == 0)
    await_from(ready.at[1], 0, 1, 2)
    start(dens_rows[0])
    greet(ready.at[3], 0, -1, h)
    greet(ready.at[2], 0, 1, h)
    get_fix.wait()

    def free_step(i, _):
        free_layer(i)
        return 0

    lax.fori_loop(0, layers, free_step, 0)

    get_ratio.wait()
    ratio_sum = ratio[0]
    for case in range(1, ratio.shape[0]):
        ratio_sum = ratio_sum + ratio[case]
    total = jnp.full((8, depth), ratio_sum.astype(jnp.float32))
    share = (SHEAR / 16.0) * (jnp.full((8, depth), ratio[h].astype(jnp.float32)) / total)


    def energy_rows(first, count, j):
        row = pl.multiple_of(j * SHORT, SHORT)
        lower = node_modes(moved, first + 1, row)
        for k in range(count):
            upper = node_modes(moved, first + k + 2, row)
            energy[first + k, pl.ds(row, SHORT), :] = share * energy_tile(lower, upper)
            lower = upper

    def energy_layers(first, count, begin, end):
        def tile(j, _):
            energy_rows(first, count, begin + 2 * j)
            energy_rows(first, count, begin + 2 * j + 1)
            return 0

        lax.fori_loop(0, (end - begin) // 2, tile, 0)

    close, wide = 2 * (1 - h), 2 * h

    def scale_rows(j, row):
        cones = cone_tiles(dens, j, row, 2)
        for n in range(2):
            weights = weight_tile(
                r * layers + half * h + j + n, nr * layers, c * rows + row, nc * rows, depth
            )
            inverse = 1.0 / weights
            physical = cones[n] * inverse
            alive = (1 - dead[j + n, pl.ds(row, TALL), :]).astype(jnp.float32)
            scale[j + n, pl.ds(row, TALL), :] = (
                alive * (-3.0 * (1.0 - 0.001)) * physical * physical * inverse
            )

    def scale_two(j):
        def tile(k, _):
            scale_rows(j, pl.multiple_of(k * TALL, TALL))
            return 0

        lax.fori_loop(0, rows // TALL, tile, 0)

    give = half * (1 - h)
    swap_a = [
        remote(
            9 + q, energy.at[pl.ds(give, half - 1), part, :],
            other.at[pl.ds(0, half - 1), part, :], 0, 0, 1 - h,
        )
        for q, part in enumerate(swap_rows)
    ]
    swap_b = [
        between(11 + q, energy.at[half - 1, part, :], other.at[half - 1, part, :], 1)
        for q, part in enumerate(swap_rows)
    ]
    rest = (half - 1) * h
    energy_layers(give, half - 1, 0, tiles - 2)
    start(swap_a[0])
    await_from(ready.at[2], 0, -1, 1)
    for entry in [dens_far[2], send_cor, dens_far[3], send_disp[0]]:
        start(entry)
    energy_layers(rest, half, 0, tiles - 2)
    start(swap_b[0])
    await_from(ready.at[3], 0, 1, 1)
    for entry in [dens_far[1], send_disp[1]]:
        start(entry)

    blank = jnp.zeros((8, depth), jnp.float32)

    @pl.when(r == nr - 1)
    def _():
        for comp in range(3):
            moved[comp, layers + 1, plane, :] = jnp.zeros((rows, depth), jnp.float32)
            moved[comp, layers + 1, pl.ds(rows, 8), :] = blank

    @pl.when(c == nc - 1)
    def _():
        col_r[...] = jnp.zeros_like(col_r)

    @pl.when(jnp.logical_not(there(-dz, 1)))
    def _():
        cor_r[...] = jnp.zeros_like(cor_r)

    @pl.when(c == 0)
    def _():
        mine[low, :] = blank
        peer[low, :] = blank

    @pl.when(c == nc - 1)
    def _():
        mine[high, :] = blank
        peer[high, :] = blank

    for ref in (dens, sens):

        @pl.when(c == 0)
        def _():
            for i in range(half + 4):
                ref[i, low, :] = blank

        @pl.when(c == nc - 1)
        def _():
            for i in range(half + 4):
                ref[i, high, :] = blank

        @pl.when(jnp.logical_not(there(-dz, 0)))
        def _():
            for i in range(2):
                ref[lz + i] = jnp.zeros((rows + 16, depth), jnp.float32)

    get_dead.wait()
    for entry in dens_rows:
        arrive(entry)
    scale_two(close)
    arrive(send_col)
    for comp in range(3):
        for i in range(layers):
            moved[comp, i + 1, pl.ds(rows, 1), :] = col_r[comp, i : i + 1, :]
    energy_layers(give, half - 1, tiles - 2, tiles)
    start(swap_a[1])
    energy_layers(rest, half, tiles - 2, tiles)
    start(swap_b[1])

    def sense(j):
        sens[2 + j, mid, :] = scale[j] * (energy[half * h + j] + other[j])

    strip_count = rows // TALL
    arrive(dens_far[0])
    arrive(dens_far[3])
    for k in range(strip_count):
        strip = (k + strip_count - c % strip_count) % strip_count
        for entry, at in ((dens_far[1], 0), (dens_far[2], strip_count - 1)):
            copy, goes, comes = entry
            arrive((copy, goes, comes & (strip == at)))
        scale_rows(wide, pl.multiple_of(strip * TALL, TALL))
    for entry in swap_a + swap_b:
        arrive(entry)

    ps, pd = pl.ds(half - (half - 2) * h, 2), pl.ds((half + 2) * h, 2)
    zs, zd = pl.ds(2 + (half - 2) * h, 2), pl.ds((half + 2) * (1 - h), 2)
    close_copies = [
        remote(13, sens.at[ps, mid, :], sens.at[pd, mid, :], 0, 0, 1 - h),
        remote(16, sens.at[ps, last, :], sens.at[pd, above, :], 0, 1, 1 - h),
        remote(17, sens.at[ps, first, :], sens.at[pd, below, :], 0, -1, 1 - h),
    ]
    low_half, high_half = pl.ds(8, tall), pl.ds(8 + tall, rows - tall)
    wide_copies = [
        flipped(18, sens.at[zs, last, :], sens.at[zd, above, :], 1),
        flipped(19, sens.at[zs, first, :], sens.at[zd, below, :], -1),
        flipped(20, sens.at[zs, low_half, :], sens.at[zd, low_half, :], 0),
        flipped(31, sens.at[zs, high_half, :], sens.at[zd, high_half, :], 0, 22),
    ]
    core_rows = pl.ds(2, half)
    row_copies = [
        remote(14, sens.at[core_rows, last, :], sens.at[core_rows, above, :], 0, 1, h),
        remote(15, sens.at[core_rows, first, :], sens.at[core_rows, below, :], 0, -1, h),
    ]
    edge_copies = [
        remote(21, mine.at[last, :], mine.at[above, :], 0, 1, h, 0),
        remote(22, mine.at[first, :], mine.at[below, :], 0, -1, h, 1),
        flipped(23, mine.at[last, :], peer.at[above, :], 1, 2),
        flipped(24, mine.at[first, :], peer.at[below, :], -1, 3),
    ]
    main_copies = [
        flipped(25 + q, mine.at[pl.ds(8 + q * tall, tall), :], peer.at[pl.ds(8 + q * tall, tall), :], 0, 4 + q)
        for q in range(CHUNKS)
    ]
    atop = (r == nr - 1) & (h == 0)
    whole = energy.at[layers - 1]
    top_copies = [
        remote(23, whole.at[top, :], peer.at[above, :], 0, 1, 1, 6),
        remote(24, whole.at[bottom, :], peer.at[below, :], 0, -1, 1, 7),
        remote(25, whole.at[halves[0], :], peer.at[pl.ds(8, tall), :], 0, 0, 1, 8),
        remote(26, whole.at[halves[1], :], peer.at[pl.ds(8 + tall, tall), :], 0, 0, 1, 9),
    ]
    top_copies = [
        (copy, goes & atop, comes & (r == nr - 1) & (h == 1)) for copy, goes, comes in top_copies
    ]
    joined = (h == 1) | (r > 0)
    edge_copies[:2] = [(copy, goes & joined, comes & joined) for copy, goes, comes in edge_copies[:2]]
    arrivals = [
        (copy, goes, comes | extra)
        for (copy, goes, comes), (_, _, extra) in zip(edge_copies[2:] + main_copies, top_copies)
    ]
    pieces = [
        [edge_copies[1], edge_copies[3], main_copies[0]],
        [edge_copies[0], edge_copies[2], main_copies[1]],
    ]

    def boundary():
        for entry in [*dens_rows, *dens_far, *send_disp, send_col, send_cor, *swap_a, *swap_b]:
            left(entry)

        arrive(send_cor)
        for comp in range(3):
            moved[comp, halo, pl.ds(rows, 1), :] = cor_r[comp : comp + 1, :]
        for q in range(CHUNKS):
            arrive(send_disp[q])

            @pl.when(joined)
            def _():
                for n in range(tall // SHORT):
                    row = q * tall + n * SHORT
                    mine[pl.ds(row + 8, SHORT), :] = share * energy_tile(
                        node_modes(moved, layers * h, row), node_modes(moved, layers * h + 1, row)
                    )

            for entry in pieces[q]:
                start(entry)
            if q == 0:
                start(wide_copies[3], c > 0)

        @pl.when(atop)
        def _():
            energy_layers(layers - 1, 1, 0, tiles)

        for entry in top_copies:
            start(entry)

    def spread():
        sense(wide)

        @pl.when(h == 0)
        def _():
            sense(1)

        @pl.when(h == 1)
        def _():
            sens[half + 1, mid, :] = scale[half - 1]

        for entry in wide_copies[:3]:
            start(entry)
        start(wide_copies[3], c == 0)
        sense(close)
        sense(close + 1)
        for entry in close_copies + row_copies:
            start(entry)

    spread()
    boundary()

    def filter_rows(j, count, row):
        cones = cone_tiles(sens, j, row, count)
        for n in range(count):
            alive = (1 - dead[j + n, pl.ds(row, TALL), :]).astype(jnp.float32)
            out[half * h + j + n, pl.ds(row, TALL), :] = alive * cones[n]

    def filter_layers(j, count):
        def tile(k, _):
            filter_rows(j, count, pl.multiple_of(k * TALL, TALL))
            return 0

        lax.fori_loop(0, rows // TALL, tile, 0)

    def hand_over(index, giver, j, count, part):
        place = out.at[pl.ds(half * giver + j, count), part, :]
        return between(index, place, place, giver, index - 17)

    early = [hand_over(27, 0, 2, half - 2, plane), hand_over(27, 1, 0, half - 3, plane)]
    strips = [pl.ds(k * TALL, TALL) for k in range(rows // TALL)]
    late = [
        [hand_over(28 + k, 0, 0, 2, strip), hand_over(28 + k, 1, half - 3, 3, strip)]
        for k, strip in enumerate(strips)
    ]
    for entry in close_copies + row_copies:
        arrive(entry)

    @pl.when(h == 0)
    def _():
        filter_layers(2, half - 2)

    @pl.when(h == 1)
    def _():
        filter_layers(0, half - 3)

    for entry in early:
        start(entry)
    for entry in close_copies + row_copies:
        left(entry)
    for entry in wide_copies:
        arrive(entry)
    for entry in wide_copies:
        left(entry)
    for entry in edge_copies + main_copies + top_copies:
        left(entry)
    b = 1 + half * h

    @pl.when(joined)
    def _():
        hold[...] = sens[b]
        sens[b] = jnp.zeros((rows + 16, depth), jnp.float32)

    def partial_layers(j, count):
        def tile(k, _):
            row = pl.multiple_of(k * TALL, TALL)
            for n, cone in enumerate(cone_tiles(sens, j, row, count)):
                out[half * h + j + n, pl.ds(row, TALL), :] = cone
            return 0

        lax.fori_loop(0, rows // TALL, tile, 0)

    @pl.when(h == 0)
    def _():
        partial_layers(0, 2)

    @pl.when(h == 1)
    def _():
        partial_layers(half - 3, 3)

    def finish_rows(pairs, row):
        for (j, reach), cone in zip(pairs, boundary_cones(sens, b, row, [p[1] for p in pairs])):
            alive = (1 - dead[j, pl.ds(row, TALL), :]).astype(jnp.float32)
            here = pl.ds(row, TALL)
            out[half * h + j, here, :] = alive * (out[half * h + j, here, :] + cone)

    for entry in edge_copies[:2] + arrivals:
        arrive(entry)

    @pl.when(joined)
    def _():
        sens[b] = hold[...] * (mine[...] + peer[...])

    for k in range(rows // TALL):

        @pl.when(h == 0)
        def _():
            finish_rows([(0, 1), (1, 2)], k * TALL)

        @pl.when(h == 1)
        def _():
            finish_rows([(half - 3, 2), (half - 2, 1), (half - 1, 0)], k * TALL)

        for entry in late[k]:
            start(entry)
    late = [entry for pair in late for entry in pair]
    for entry in early + late:
        left(entry)
    for entry in early + late:
        arrive(entry)


def shards(density, void_mask, fixed_mask, displacement, load_ratio):
    layers, rows, depth = density.shape
    half = layers // 2
    f32 = jnp.float32
    hbm = pl.BlockSpec(memory_space=pl.ANY)
    return pl.pallas_call(
        kernel,
        out_shape=pltpu.VMEM(density.shape, f32),
        in_specs=[hbm] * 5,
        out_specs=pl.BlockSpec(memory_space=pltpu.VMEM),
        scratch_shapes=[
            pltpu.VMEM((3, layers + 2, rows + 8, depth), f32),
            pltpu.VMEM((layers, rows, depth), jnp.int32),
            pltpu.VMEM((3, layers, depth), f32),
            pltpu.VMEM((3, layers, depth), f32),
            pltpu.VMEM((8, depth), f32),
            pltpu.VMEM((8, depth), f32),
            pltpu.VMEM((half + 4, rows + 16, depth), f32),
            pltpu.VMEM((half, rows, depth), jnp.int32),
            pltpu.VMEM((half, rows, depth), f32),
            pltpu.VMEM((layers, rows, depth), f32),
            pltpu.VMEM((half, rows, depth), f32),
            pltpu.VMEM((half + 4, rows + 16, depth), f32),
            pltpu.VMEM((rows + 16, depth), f32),
            pltpu.VMEM((rows + 16, depth), f32),
            pltpu.VMEM((rows + 16, depth), f32),
            pltpu.SMEM(load_ratio.shape, load_ratio.dtype),
            pltpu.VMEM((2, rows, depth), f32),
            pltpu.VMEM((3, layers, 1, depth), f32),
            pltpu.VMEM((layers, 1, depth), jnp.int32),
            pltpu.SemaphoreType.DMA((8,)),
            pltpu.SemaphoreType.DMA((N_SEND,)),
            pltpu.SemaphoreType.DMA((N_RECV,)),
            pltpu.SemaphoreType.REGULAR((4,)),
        ],
        compiler_params=pltpu.CompilerParams(collective_id=0, has_side_effects=True),
    )(load_ratio, density, void_mask, fixed_mask, displacement)


def solution(mesh):
    placed = (
        P(("parts", "gz"), "gy", None),
        P(("parts", "gz"), "gy", None),
        P(("parts", "gz"), "gy", None),
        P("lc", None, ("parts", "gz"), "gy", None),
        P("parts"),
    )
    return jax.shard_map(
        shards,
        mesh=mesh,
        in_specs=placed,
        out_specs=P(("parts", "gz"), "gy", None),
        check_vma=False,
    )
```

```python
import math

import jax
import jax.numpy as jnp
from jax import lax
from jax.experimental import pallas as pl
from jax.experimental.pallas import tpu as pltpu
from jax.sharding import PartitionSpec as P

MESH = pl.DeviceIdType.MESH
POISSON = 0.3
FACTOR = 1.0 / ((1.0 + POISSON) * (1.0 - 2.0 * POISSON))
LAMBDA = POISSON * FACTOR
SHEAR = (0.5 - POISSON) * FACTOR
RATIO = LAMBDA / SHEAR
W = [2.5 - math.sqrt(d) for d in range(7)]
CHUNKS = 2
EDGE = 2
N_SEND = 19
N_RECV = 26
TALL = 32
SHORT = 8


def layer_classes(q0, q1, q2, q4, q5):
    p0 = W[0] * q0 + W[1] * q1 + W[2] * q2 + W[4] * q4 + W[5] * q5
    p1 = W[1] * q0 + W[2] * q1 + W[3] * q2 + W[5] * q4 + W[6] * q5
    p2 = W[4] * q0 + W[5] * q1 + W[6] * q2
    return p0, p1, p2


def lane_index(shape):
    return lax.broadcasted_iota(jnp.int32, shape, len(shape) - 1)


def lane_pair(field, step):
    depth = field.shape[-1]
    lane = lane_index(field.shape)
    after = jnp.where(lane < depth - step, pltpu.roll(field, depth - step, 1), 0.0)
    before = jnp.where(lane >= step, pltpu.roll(field, step, 1), 0.0)
    return after + before


def cone_tiles(ref, layer, row, count):
    window = TALL + 16
    f = [ref[layer + k, pl.ds(row, window), :] for k in range(count + 4)]
    mid = slice(8, 8 + TALL)

    def pair(t, step):
        return (pltpu.roll(t, step, 0) + pltpu.roll(t, window - step, 0))[mid]

    result = []
    for k in range(count):
        x0, x1, x2 = f[k + 2], f[k + 1] + f[k + 3], f[k] + f[k + 4]
        q0 = x0[mid]
        q1 = x1[mid] + pair(x0, 1)
        q2 = pair(x1, 1)
        q4 = x2[mid] + pair(x0, 2)
        q5 = pair(x2, 1) + pair(x1, 2)
        p0, p1, p2 = layer_classes(q0, q1, q2, q4, q5)
        result.append(p0 + lane_pair(p1, 1) + lane_pair(p2, 2))
    return result


def boundary_cones(ref, layer, row, reaches):
    window = TALL + 16
    t = ref[layer, pl.ds(row, window), :]
    mid = slice(8, 8 + TALL)
    t0 = t[mid]
    t1, t2 = [
        (pltpu.roll(t, step, 0) + pltpu.roll(t, window - step, 0))[mid] for step in (1, 2)
    ]
    result = []
    for reach in reaches:
        if reach == 0:
            p0 = W[0] * t0 + W[1] * t1 + W[4] * t2
            p1 = W[1] * t0 + W[2] * t1 + W[5] * t2
            p2 = W[4] * t0 + W[5] * t1
        elif reach == 1:
            p0 = W[1] * t0 + W[2] * t1 + W[5] * t2
            p1 = W[2] * t0 + W[3] * t1 + W[6] * t2
            p2 = W[5] * t0 + W[6] * t1
        else:
            p0, p1, p2 = W[4] * t0 + W[5] * t1, W[5] * t0 + W[6] * t1, None
        total = p0 + lane_pair(p1, 1)
        result.append(total if p2 is None else total + lane_pair(p2, 2))
    return result


def present(position, total, step):
    before = (position >= step).astype(jnp.float32)
    return before + (position + step < total).astype(jnp.float32)


def weight_tile(layer, layers, row, rows, depth):
    shape = (TALL, depth)
    sub = lax.broadcasted_iota(jnp.int32, shape, 0) + row
    spot = jnp.full(shape, layer, jnp.int32)
    nx1, nx2 = present(spot, layers, 1), present(spot, layers, 2)
    ny1, ny2 = present(sub, rows, 1), present(sub, rows, 2)
    one = jnp.ones(shape, jnp.float32)
    p0, p1, p2 = layer_classes(one, nx1 + ny1, nx1 * ny1, nx2 + ny2, nx2 * ny1 + nx1 * ny2)
    lane = lane_index(shape)
    return p0 + present(lane, depth, 1) * p1 + present(lane, depth, 2) * p2


def node_modes(ref, layer, row):
    result = []
    for comp in range(3):
        t = ref[comp, layer, pl.ds(row, SHORT + 8), :]
        depth, window = t.shape[-1], t.shape[0]
        here, after = t[0:SHORT], pltpu.roll(t, window - 1, 0)[0:SHORT]
        s, d = here + after, after - here
        inner = lane_index(s.shape) < depth - 1
        sn = jnp.where(inner, pltpu.roll(s, depth - 1, 1), 0.0)
        dn = jnp.where(inner, pltpu.roll(d, depth - 1, 1), 0.0)
        result.append((s + sn, sn - s, d + dn, dn - d))
    return result


def energy_tile(lower, upper):
    modes = []
    for a, b in zip(lower, upper):
        modes.append(
            {
                "x": b[0] - a[0],
                "z": a[1] + b[1],
                "y": a[2] + b[2],
                "yz": a[3] + b[3],
                "xz": b[1] - a[1],
                "xy": b[2] - a[2],
                "xyz": b[3] - a[3],
            }
        )
    u, v, w = modes
    sq = lambda t: t * t
    trace = sq(u["x"] + v["y"] + w["z"])
    normal = sq(u["x"]) + sq(v["y"]) + sq(w["z"])
    bend = sq(u["xy"]) + sq(u["xz"]) + sq(v["xy"]) + sq(v["yz"]) + sq(w["yz"]) + sq(w["xz"])
    cross = v["xy"] * w["xz"] + u["xy"] * w["yz"] + u["xz"] * v["yz"]
    shear = sq(u["y"] + v["x"]) + sq(u["z"] + w["x"]) + sq(v["z"] + w["y"])
    pair = v["xz"] + w["xy"]
    twist = u["yz"] * (u["yz"] + pair) + v["xz"] * pair + sq(w["xy"])
    cubic = sq(u["xyz"]) + sq(v["xyz"]) + sq(w["xyz"])
    return (
        RATIO * trace
        + 2.0 * normal
        + (1.0 + RATIO / 3.0) * bend
        + (2.0 * RATIO / 3.0) * cross
        + shear
        + (2.0 / 3.0) * twist
        + ((RATIO + 4.0) / 9.0) * cubic
    )


def kernel(
    ratio_in, density, void, fixed, disp, out,
    moved, fix, col_s, col_r, cor_s, cor_r, dens, dead, scale, energy, other, sens, mine, peer, hold, ratio,
    border, rim, held, local, send, recv, ready,
):
    layers, rows, depth = density.shape
    half = layers // 2
    r, c, h = lax.axis_index("gz"), lax.axis_index("gy"), lax.axis_index("lc")
    nr, nc = lax.axis_size("gz"), lax.axis_size("gy")
    dz = 1 - 2 * h
    mid = pl.ds(8, rows)
    low, high = pl.ds(0, 8), pl.ds(rows + 8, 8)

    def there(step_z, step_y):
        z, y = r + step_z, c + step_y
        return (z >= 0) & (z < nr) & (y >= 0) & (y < nc)

    def remote(index, src, dst, step_z, step_y, core, slot=None):
        copy = pltpu.make_async_remote_copy(
            src_ref=src, dst_ref=dst, send_sem=send.at[index if slot is None else slot],
            recv_sem=recv.at[index],
            device_id={"gz": r + step_z, "gy": c + step_y, "lc": core}, device_id_type=MESH,
        )
        goes, comes = there(step_z, step_y), there(-step_z, -step_y)
        return copy, goes, comes

    def between(index, src, dst, giver, slot=None):
        taker = 1 - giver
        copy, goes, comes = remote(index, src, dst, 0, 0, taker, slot)
        return copy, goes & (h == giver), comes & (h == taker)

    def flipped(index, src, dst, step_y, slot=None):
        copy, goes, _ = remote(index, src, dst, -dz, step_y, 1 - h, slot)
        return copy, goes, there(-dz, -step_y)

    def start(entry, when=True):
        copy, goes, _ = entry
        pl.when(goes & when)(copy.start)

    def arrive(entry):
        copy, _, comes = entry
        pl.when(comes)(copy.wait_recv)

    def left(entry):
        copy, goes, _ = entry
        pl.when(goes)(copy.wait_send)

    l0, b0 = half // 2 * (1 - h), half // 2 * h
    keep = half + 2
    lz, sb = (half + 2) * h, (layers - 2) * (1 - h)
    plane = pl.ds(0, rows)
    given, halo = (layers - 1) * (1 - h), (layers + 1) * h
    get_disp = pltpu.make_async_copy(
        disp.at[0], moved.at[:, pl.ds(1, layers), plane, :], local.at[0]
    )
    get_fix = pltpu.make_async_copy(fixed, fix, local.at[1])
    get_rim = pltpu.make_async_copy(disp.at[0, :, :, pl.ds(0, 1), :], rim, local.at[6])
    get_held = pltpu.make_async_copy(fixed.at[:, pl.ds(0, 1), :], held, local.at[7])
    get_dens = pltpu.make_async_copy(
        density.at[pl.ds(b0, keep)], dens.at[pl.ds(l0, keep), mid, :], local.at[2]
    )
    get_dead = pltpu.make_async_copy(void.at[pl.ds(half * h, half)], dead, local.at[3])
    get_ratio = pltpu.make_async_copy(ratio_in, ratio, local.at[4])
    get_border = pltpu.make_async_copy(density.at[pl.ds(sb, 2)], border, local.at[5])
    for copy in (get_rim, get_held, get_border, get_dens, get_disp, get_fix, get_ratio, get_dead):
        copy.start()

    barrier = pltpu.get_barrier_semaphore()
    def greet(semaphore, step_z, step_y, core):
        @pl.when(there(step_z, step_y))
        def _():
            pl.semaphore_signal(
                semaphore, inc=1,
                device_id={"gz": r + step_z, "gy": c + step_y, "lc": core},
                device_id_type=MESH,
            )

    flag = lambda value: value.astype(jnp.int32)

    def await_from(semaphore, step_z, step_y, count):
        @pl.when(there(step_z, step_y))
        def _():
            pl.semaphore_wait(semaphore, count)

    for core in (h, 1 - h):
        greet(barrier, 1, 0, core)
        greet(barrier, 0, 1, core)
    greet(barrier, 0, 0, 1 - h)

    near, far = pl.ds(l0, keep), pl.ds(lz, 2)
    zs, zd = pl.ds(2 + (half - 2) * h, 2), pl.ds((half + 2) * (1 - h), 2)
    tiles = rows // SHORT
    head = (tiles - 2) * SHORT
    swap_rows = [pl.ds(0, head), pl.ds(head, rows - head)]
    top, bottom = pl.ds(rows - EDGE, EDGE), pl.ds(0, EDGE)
    above, below = pl.ds(8 - EDGE, EDGE), pl.ds(rows + 8, EDGE)
    last, first = pl.ds(rows + 8 - EDGE, EDGE), pl.ds(8, EDGE)
    dens_rows = [
        remote(1, dens.at[near, last, :], dens.at[near, above, :], 0, 1, h),
        remote(2, dens.at[near, first, :], dens.at[near, below, :], 0, -1, h),
    ]
    dens_far = [
        remote(0, border, dens.at[far, mid, :], dz, 0, h),
        flipped(3, dens.at[zs, last, :], dens.at[zd, above, :], 1),
        flipped(4, dens.at[zs, first, :], dens.at[zd, below, :], -1),
    ]

    def free_layer(i):
        free = (1 - fix[i]).astype(jnp.float32)
        for comp in range(3):
            moved[comp, i + 1, plane, :] = moved[comp, i + 1, plane, :] * free

    tall = rows // CHUNKS
    parts = [pl.ds(0, tall + SHORT), pl.ds(tall + SHORT, rows - tall - SHORT)]
    halves = [pl.ds(q * tall, tall) for q in range(CHUNKS)]
    send_disp = [
        remote(5 + q, moved.at[:, given + 1, part, :], moved.at[:, halo, part, :], dz, 0, h)
        for q, part in enumerate(parts)
    ]
    send_col = remote(7, col_s, col_r, 0, -1, h)
    send_cor = remote(8, cor_s, cor_r, dz, -1, h)
    pl.semaphore_wait(barrier, 2 * (flag(r > 0) + flag(c > 0)) + 1)
    for core in (h, 1 - h):
        greet(ready.at[0], -1, 0, core)
        greet(ready.at[1], 0, -1, core)
    get_rim.wait()
    get_held.wait()
    for i in range(layers):
        free = (1 - held[i]).astype(jnp.float32)
        for comp in range(3):
            col_s[comp, i : i + 1, :] = rim[comp, i] * free
    start(send_col)
    for comp in range(3):
        cor_s[comp : comp + 1, :] = rim[comp, given] * (1 - held[given]).astype(jnp.float32)
    get_border.wait()
    start(dens_far[0], h == 1)
    get_dens.wait()
    start(dens_rows[1])
    get_disp.wait()
    await_from(ready.at[1], 0, 1, 2)
    greet(ready.at[2], 0, 1, h)
    start(dens_rows[0])
    start(dens_far[1], h == 0)
    await_from(ready.at[0], 1, 0, 2)
    greet(ready.at[3], 0, -1, h)
    start(dens_far[2], h == 1)
    start(dens_far[0], h == 0)
    start(send_cor, h == 0)
    get_fix.wait()

    def free_step(i, _):
        free_layer(i)
        return 0

    lax.fori_loop(0, layers, free_step, 0)
    start(send_disp[0])
    await_from(ready.at[2], 0, -1, 1)
    start(dens_far[2], h == 0)
    start(send_cor, h == 1)

    get_ratio.wait()
    ratio_sum = ratio[0]
    for case in range(1, ratio.shape[0]):
        ratio_sum = ratio_sum + ratio[case]
    total = jnp.full((8, depth), ratio_sum.astype(jnp.float32))
    share = (SHEAR / 16.0) * (jnp.full((8, depth), ratio[h].astype(jnp.float32)) / total)


    def energy_rows(first, count, j):
        row = pl.multiple_of(j * SHORT, SHORT)
        lower = node_modes(moved, first + 1, row)
        for k in range(count):
            upper = node_modes(moved, first + k + 2, row)
            energy[first + k, pl.ds(row, SHORT), :] = share * energy_tile(lower, upper)
            lower = upper

    def energy_layers(first, count, begin, end):
        def tile(j, _):
            energy_rows(first, count, begin + 2 * j)
            energy_rows(first, count, begin + 2 * j + 1)
            return 0

        lax.fori_loop(0, (end - begin) // 2, tile, 0)

    close, wide = 2 * (1 - h), 2 * h

    def scale_rows(j, row):
        cones = cone_tiles(dens, j, row, 2)
        for n in range(2):
            weights = weight_tile(
                r * layers + half * h + j + n, nr * layers, c * rows + row, nc * rows, depth
            )
            inverse = 1.0 / weights
            physical = cones[n] * inverse
            alive = (1 - dead[j + n, pl.ds(row, TALL), :]).astype(jnp.float32)
            scale[j + n, pl.ds(row, TALL), :] = (
                alive * (-3.0 * (1.0 - 0.001)) * physical * physical * inverse
            )

    def scale_two(j):
        def tile(k, _):
            scale_rows(j, pl.multiple_of(k * TALL, TALL))
            return 0

        lax.fori_loop(0, rows // TALL, tile, 0)

    give = half * (1 - h)
    swap_a = [
        remote(
            9, energy.at[pl.ds(give, half - 1), part, :],
            other.at[pl.ds(0, half - 1), part, :], 0, 0, 1 - h,
        )
        for q, part in enumerate(swap_rows)
    ]
    swap_b = [
        between(10, energy.at[half - 1, part, :], other.at[half - 1, part, :], 1)
        for q, part in enumerate(swap_rows)
    ]
    swap_whole = [
        remote(9, energy.at[pl.ds(give, half - 1)], other.at[pl.ds(0, half - 1)], 0, 0, 1 - h),
        between(10, energy.at[half - 1], other.at[half - 1], 1),
    ]
    rest = (half - 1) * h
    energy_layers(give, half - 1, 0, tiles - 2)
    start(swap_a[0])
    energy_layers(rest, half, 0, tiles - 2)
    start(swap_b[0])
    await_from(ready.at[3], 0, 1, 1)
    start(dens_far[1], h == 1)
    start(send_disp[1])

    blank = jnp.zeros((8, depth), jnp.float32)

    @pl.when(r == nr - 1)
    def _():
        for comp in range(3):
            moved[comp, layers + 1, plane, :] = jnp.zeros((rows, depth), jnp.float32)
            moved[comp, layers + 1, pl.ds(rows, 8), :] = blank

    @pl.when(c == nc - 1)
    def _():
        col_r[...] = jnp.zeros_like(col_r)

    @pl.when(jnp.logical_not(there(-dz, 1)))
    def _():
        cor_r[...] = jnp.zeros_like(cor_r)

    @pl.when(c == 0)
    def _():
        mine[low, :] = blank
        peer[low, :] = blank

    @pl.when(c == nc - 1)
    def _():
        mine[high, :] = blank
        peer[high, :] = blank

    for ref in (dens, sens):

        @pl.when(c == 0)
        def _():
            for i in range(half + 4):
                ref[i, low, :] = blank

        @pl.when(c == nc - 1)
        def _():
            for i in range(half + 4):
                ref[i, high, :] = blank

        @pl.when(jnp.logical_not(there(-dz, 0)))
        def _():
            for i in range(2):
                ref[lz + i] = jnp.zeros((rows + 16, depth), jnp.float32)

    get_dead.wait()
    for entry in dens_rows:
        arrive(entry)
    scale_two(close)
    arrive(send_col)
    for comp in range(3):
        for i in range(layers):
            moved[comp, i + 1, pl.ds(rows, 1), :] = col_r[comp, i : i + 1, :]
    energy_layers(give, half - 1, tiles - 2, tiles)
    start(swap_a[1])
    energy_layers(rest, half, tiles - 2, tiles)
    start(swap_b[1])

    def sense(j):
        sens[2 + j, mid, :] = scale[j] * (energy[half * h + j] + other[j])

    strip_count = rows // TALL
    arrive(dens_far[0])
    for k in range(strip_count):
        strip = (k + strip_count - c % strip_count) % strip_count
        for entry, at in ((dens_far[1], 0), (dens_far[2], strip_count - 1)):
            copy, goes, comes = entry
            arrive((copy, goes, comes & (strip == at)))
        scale_rows(wide, pl.multiple_of(strip * TALL, TALL))
    for entry in swap_whole:
        arrive(entry)

    ps, pd = pl.ds(half - (half - 2) * h, 2), pl.ds((half + 2) * h, 2)
    close_copies = [
        remote(11, sens.at[ps, mid, :], sens.at[pd, mid, :], 0, 0, 1 - h),
        remote(14, sens.at[ps, last, :], sens.at[pd, above, :], 0, 1, 1 - h),
        remote(15, sens.at[ps, first, :], sens.at[pd, below, :], 0, -1, 1 - h),
    ]
    low_half, high_half = pl.ds(8, tall), pl.ds(8 + tall, rows - tall)
    wide_copies = [
        flipped(16, sens.at[zs, last, :], sens.at[zd, above, :], 1),
        flipped(17, sens.at[zs, first, :], sens.at[zd, below, :], -1),
        flipped(18, sens.at[zs, low_half, :], sens.at[zd, low_half, :], 0),
        flipped(18, sens.at[zs, high_half, :], sens.at[zd, high_half, :], 0),
    ]
    wide_whole = [*wide_copies[:2], flipped(18, sens.at[zs, mid, :], sens.at[zd, mid, :], 0)]
    core_rows = pl.ds(2, half)
    row_copies = [
        remote(12, sens.at[core_rows, last, :], sens.at[core_rows, above, :], 0, 1, h),
        remote(13, sens.at[core_rows, first, :], sens.at[core_rows, below, :], 0, -1, h),
    ]
    edge_copies = [
        remote(19, mine.at[last, :], mine.at[above, :], 0, 1, h, 0),
        remote(20, mine.at[first, :], mine.at[below, :], 0, -1, h, 1),
        flipped(21, mine.at[last, :], peer.at[above, :], 1, 2),
        flipped(22, mine.at[first, :], peer.at[below, :], -1, 3),
    ]
    main_copies = [
        flipped(23, mine.at[pl.ds(8 + q * tall, tall), :], peer.at[pl.ds(8 + q * tall, tall), :], 0, 4)
        for q in range(CHUNKS)
    ]
    main_whole = flipped(23, mine.at[mid, :], peer.at[mid, :], 0, 4)
    atop = (r == nr - 1) & (h == 0)
    whole = energy.at[layers - 1]
    top_copies = [
        remote(21, whole.at[top, :], peer.at[above, :], 0, 1, 1, 6),
        remote(22, whole.at[bottom, :], peer.at[below, :], 0, -1, 1, 7),
        remote(23, whole.at[halves[0], :], peer.at[pl.ds(8, tall), :], 0, 0, 1, 8),
        remote(23, whole.at[halves[1], :], peer.at[pl.ds(8 + tall, tall), :], 0, 0, 1, 8),
    ]
    top_copies = [
        (copy, goes & atop, comes & (r == nr - 1) & (h == 1)) for copy, goes, comes in top_copies
    ]
    top_whole, _, _ = remote(23, whole.at[plane, :], peer.at[mid, :], 0, 0, 1, 8)
    top_whole = [*top_copies[:2], (top_whole, atop, False)]
    joined = (h == 1) | (r > 0)
    edge_copies[:2] = [(copy, goes & joined, comes & joined) for copy, goes, comes in edge_copies[:2]]
    arrivals = [
        (copy, goes, comes | extra)
        for (copy, goes, comes), (_, _, extra) in zip(edge_copies[2:] + [main_whole], top_copies)
    ]
    pieces = [
        [edge_copies[1], edge_copies[3], main_copies[0]],
        [edge_copies[0], edge_copies[2], main_copies[1]],
    ]

    def boundary():
        for entry in [*dens_rows, *dens_far, *send_disp, send_col, send_cor, *swap_whole]:
            left(entry)

        arrive(send_cor)
        for comp in range(3):
            moved[comp, halo, pl.ds(rows, 1), :] = cor_r[comp : comp + 1, :]
        for q in range(CHUNKS):
            arrive(send_disp[q])

            @pl.when(joined)
            def _():
                for n in range(tall // SHORT):
                    row = q * tall + n * SHORT
                    mine[pl.ds(row + 8, SHORT), :] = share * energy_tile(
                        node_modes(moved, layers * h, row), node_modes(moved, layers * h + 1, row)
                    )

            for entry in pieces[q]:
                start(entry)
            if q == 0:
                start(wide_copies[3], c > 0)

        @pl.when(atop)
        def _():
            energy_layers(layers - 1, 1, 0, tiles)

        for entry in top_copies:
            start(entry)

    def spread():
        sense(wide)

        @pl.when(h == 0)
        def _():
            sense(1)

        @pl.when(h == 1)
        def _():
            sens[half + 1, mid, :] = scale[half - 1]

        for entry in wide_copies[:3]:
            start(entry)
        start(wide_copies[3], c == 0)
        sense(close)
        sense(close + 1)
        for entry in close_copies + row_copies:
            start(entry)

    spread()
    boundary()

    def filter_rows(j, count, row):
        cones = cone_tiles(sens, j, row, count)
        for n in range(count):
            alive = (1 - dead[j + n, pl.ds(row, TALL), :]).astype(jnp.float32)
            out[half * h + j + n, pl.ds(row, TALL), :] = alive * cones[n]

    def filter_layers(j, count):
        def tile(k, _):
            filter_rows(j, count, pl.multiple_of(k * TALL, TALL))
            return 0

        lax.fori_loop(0, rows // TALL, tile, 0)

    def partial_layers(j, count):
        def tile(k, _):
            row = pl.multiple_of(k * TALL, TALL)
            for n, cone in enumerate(cone_tiles(sens, j, row, count)):
                out[half * h + j + n, pl.ds(row, TALL), :] = cone
            return 0

        lax.fori_loop(0, rows // TALL, tile, 0)

    def hand_over(index, giver, j, count, part):
        place = out.at[pl.ds(half * giver + j, count), part, :]
        return between(index, place, place, giver, index - 15)

    early = [hand_over(24, 0, 2, half - 2, plane), hand_over(24, 1, 0, half - 3, plane)]
    strips = [pl.ds(k * TALL, TALL) for k in range(rows // TALL)]
    late = [
        [hand_over(25, 0, 0, 2, strip), hand_over(25, 1, half - 3, 3, strip)]
        for k, strip in enumerate(strips)
    ]
    for entry in close_copies + row_copies:
        arrive(entry)

    @pl.when(h == 0)
    def _():
        filter_layers(2, half - 2)

    @pl.when(h == 1)
    def _():
        filter_layers(0, half - 3)

    for entry in early:
        start(entry)
    for entry in close_copies + row_copies + wide_whole:
        left(entry)
    b = 1 + half * h

    def set_aside():
        hold[...] = sens[b]
        sens[b] = jnp.zeros((rows + 16, depth), jnp.float32)

    @pl.when(h == 1)
    def _():
        set_aside()
        partial_layers(half - 3, 1)

    for entry in wide_whole:
        arrive(entry)
    for entry in edge_copies + [main_whole] + top_whole:
        left(entry)
    pl.when((h == 0) & joined)(set_aside)

    @pl.when(h == 0)
    def _():
        partial_layers(0, 2)

    @pl.when(h == 1)
    def _():
        partial_layers(half - 2, 2)

    def finish_rows(pairs, row):
        for (j, reach), cone in zip(pairs, boundary_cones(sens, b, row, [p[1] for p in pairs])):
            alive = (1 - dead[j, pl.ds(row, TALL), :]).astype(jnp.float32)
            here = pl.ds(row, TALL)
            out[half * h + j, here, :] = alive * (out[half * h + j, here, :] + cone)

    for entry in edge_copies[:2] + arrivals:
        arrive(entry)

    @pl.when(joined)
    def _():
        sens[b] = hold[...] * (mine[...] + peer[...])

    for k in range(rows // TALL):

        @pl.when(h == 0)
        def _():
            finish_rows([(0, 1), (1, 2)], k * TALL)

        @pl.when(h == 1)
        def _():
            finish_rows([(half - 3, 2), (half - 2, 1), (half - 1, 0)], k * TALL)

        for entry in late[k]:
            start(entry)
    late = [hand_over(25, 0, 0, 2, plane), hand_over(25, 1, half - 3, 3, plane)]
    for entry in early + late:
        left(entry)
    for entry in early + late:
        arrive(entry)


def shards(density, void_mask, fixed_mask, displacement, load_ratio):
    layers, rows, depth = density.shape
    half = layers // 2
    f32 = jnp.float32
    hbm = pl.BlockSpec(memory_space=pl.ANY)
    return pl.pallas_call(
        kernel,
        out_shape=pltpu.VMEM(density.shape, f32),
        in_specs=[hbm] * 5,
        out_specs=pl.BlockSpec(memory_space=pltpu.VMEM),
        scratch_shapes=[
            pltpu.VMEM((3, layers + 2, rows + 8, depth), f32),
            pltpu.VMEM((layers, rows, depth), jnp.int32),
            pltpu.VMEM((3, layers, depth), f32),
            pltpu.VMEM((3, layers, depth), f32),
            pltpu.VMEM((8, depth), f32),
            pltpu.VMEM((8, depth), f32),
            pltpu.VMEM((half + 4, rows + 16, depth), f32),
            pltpu.VMEM((half, rows, depth), jnp.int32),
            pltpu.VMEM((half, rows, depth), f32),
            pltpu.VMEM((layers, rows, depth), f32),
            pltpu.VMEM((half, rows, depth), f32),
            pltpu.VMEM((half + 4, rows + 16, depth), f32),
            pltpu.VMEM((rows + 16, depth), f32),
            pltpu.VMEM((rows + 16, depth), f32),
            pltpu.VMEM((rows + 16, depth), f32),
            pltpu.SMEM(load_ratio.shape, load_ratio.dtype),
            pltpu.VMEM((2, rows, depth), f32),
            pltpu.VMEM((3, layers, 1, depth), f32),
            pltpu.VMEM((layers, 1, depth), jnp.int32),
            pltpu.SemaphoreType.DMA((8,)),
            pltpu.SemaphoreType.DMA((N_SEND,)),
            pltpu.SemaphoreType.DMA((N_RECV,)),
            pltpu.SemaphoreType.REGULAR((4,)),
        ],
        compiler_params=pltpu.CompilerParams(collective_id=0, has_side_effects=True),
    )(load_ratio, density, void_mask, fixed_mask, displacement)


def solution(mesh):
    placed = (
        P(("parts", "gz"), "gy", None),
        P(("parts", "gz"), "gy", None),
        P(("parts", "gz"), "gy", None),
        P("lc", None, ("parts", "gz"), "gy", None),
        P("parts"),
    )
    return jax.shard_map(
        shards,
        mesh=mesh,
        in_specs=placed,
        out_specs=P(("parts", "gz"), "gy", None),
        check_vma=False,
    )
```

```python
import math

import jax
import jax.numpy as jnp
from jax import lax
from jax.experimental import pallas as pl
from jax.experimental.pallas import tpu as pltpu
from jax.sharding import PartitionSpec as P

MESH = pl.DeviceIdType.MESH
POISSON = 0.3
FACTOR = 1.0 / ((1.0 + POISSON) * (1.0 - 2.0 * POISSON))
LAMBDA = POISSON * FACTOR
SHEAR = (0.5 - POISSON) * FACTOR
RATIO = LAMBDA / SHEAR
W = [2.5 - math.sqrt(d) for d in range(7)]
CHUNKS = 2
EDGE = 2
N_SEND = 19
N_RECV = 26
TALL = 32
SHORT = 8


def layer_classes(q0, q1, q2, q4, q5):
    p0 = W[0] * q0 + W[1] * q1 + W[2] * q2 + W[4] * q4 + W[5] * q5
    p1 = W[1] * q0 + W[2] * q1 + W[3] * q2 + W[5] * q4 + W[6] * q5
    p2 = W[4] * q0 + W[5] * q1 + W[6] * q2
    return p0, p1, p2


def lane_index(shape):
    return lax.broadcasted_iota(jnp.int32, shape, len(shape) - 1)


def lane_pair(field, step):
    depth = field.shape[-1]
    lane = lane_index(field.shape)
    after = jnp.where(lane < depth - step, pltpu.roll(field, depth - step, 1), 0.0)
    before = jnp.where(lane >= step, pltpu.roll(field, step, 1), 0.0)
    return after + before


def cone_tiles(ref, layer, row, count):
    window = TALL + 16
    f = [ref[layer + k, pl.ds(row, window), :] for k in range(count + 4)]
    mid = slice(8, 8 + TALL)

    def pair(t, step):
        return (pltpu.roll(t, step, 0) + pltpu.roll(t, window - step, 0))[mid]

    result = []
    for k in range(count):
        x0, x1, x2 = f[k + 2], f[k + 1] + f[k + 3], f[k] + f[k + 4]
        q0 = x0[mid]
        q1 = x1[mid] + pair(x0, 1)
        q2 = pair(x1, 1)
        q4 = x2[mid] + pair(x0, 2)
        q5 = pair(x2, 1) + pair(x1, 2)
        p0, p1, p2 = layer_classes(q0, q1, q2, q4, q5)
        result.append(p0 + lane_pair(p1, 1) + lane_pair(p2, 2))
    return result


def boundary_cones(ref, layer, row, reaches):
    window = TALL + 16
    t = ref[layer, pl.ds(row, window), :]
    mid = slice(8, 8 + TALL)
    t0 = t[mid]
    t1, t2 = [
        (pltpu.roll(t, step, 0) + pltpu.roll(t, window - step, 0))[mid] for step in (1, 2)
    ]
    result = []
    for reach in reaches:
        if reach == 0:
            p0 = W[0] * t0 + W[1] * t1 + W[4] * t2
            p1 = W[1] * t0 + W[2] * t1 + W[5] * t2
            p2 = W[4] * t0 + W[5] * t1
        elif reach == 1:
            p0 = W[1] * t0 + W[2] * t1 + W[5] * t2
            p1 = W[2] * t0 + W[3] * t1 + W[6] * t2
            p2 = W[5] * t0 + W[6] * t1
        else:
            p0, p1, p2 = W[4] * t0 + W[5] * t1, W[5] * t0 + W[6] * t1, None
        total = p0 + lane_pair(p1, 1)
        result.append(total if p2 is None else total + lane_pair(p2, 2))
    return result


def present(position, total, step):
    before = (position >= step).astype(jnp.float32)
    return before + (position + step < total).astype(jnp.float32)


def weight_tile(layer, layers, row, rows, depth):
    shape = (TALL, depth)
    sub = lax.broadcasted_iota(jnp.int32, shape, 0) + row
    spot = jnp.full(shape, layer, jnp.int32)
    nx1, nx2 = present(spot, layers, 1), present(spot, layers, 2)
    ny1, ny2 = present(sub, rows, 1), present(sub, rows, 2)
    one = jnp.ones(shape, jnp.float32)
    p0, p1, p2 = layer_classes(one, nx1 + ny1, nx1 * ny1, nx2 + ny2, nx2 * ny1 + nx1 * ny2)
    lane = lane_index(shape)
    return p0 + present(lane, depth, 1) * p1 + present(lane, depth, 2) * p2


def node_modes(ref, layer, row):
    result = []
    for comp in range(3):
        t = ref[comp, layer, pl.ds(row, SHORT + 8), :]
        depth, window = t.shape[-1], t.shape[0]
        here, after = t[0:SHORT], pltpu.roll(t, window - 1, 0)[0:SHORT]
        s, d = here + after, after - here
        inner = lane_index(s.shape) < depth - 1
        sn = jnp.where(inner, pltpu.roll(s, depth - 1, 1), 0.0)
        dn = jnp.where(inner, pltpu.roll(d, depth - 1, 1), 0.0)
        result.append((s + sn, sn - s, d + dn, dn - d))
    return result


def energy_tile(lower, upper):
    modes = []
    for a, b in zip(lower, upper):
        modes.append(
            {
                "x": b[0] - a[0],
                "z": a[1] + b[1],
                "y": a[2] + b[2],
                "yz": a[3] + b[3],
                "xz": b[1] - a[1],
                "xy": b[2] - a[2],
                "xyz": b[3] - a[3],
            }
        )
    u, v, w = modes
    sq = lambda t: t * t
    trace = sq(u["x"] + v["y"] + w["z"])
    normal = sq(u["x"]) + sq(v["y"]) + sq(w["z"])
    bend = sq(u["xy"]) + sq(u["xz"]) + sq(v["xy"]) + sq(v["yz"]) + sq(w["yz"]) + sq(w["xz"])
    cross = v["xy"] * w["xz"] + u["xy"] * w["yz"] + u["xz"] * v["yz"]
    shear = sq(u["y"] + v["x"]) + sq(u["z"] + w["x"]) + sq(v["z"] + w["y"])
    pair = v["xz"] + w["xy"]
    twist = u["yz"] * (u["yz"] + pair) + v["xz"] * pair + sq(w["xy"])
    cubic = sq(u["xyz"]) + sq(v["xyz"]) + sq(w["xyz"])
    return (
        RATIO * trace
        + 2.0 * normal
        + (1.0 + RATIO / 3.0) * bend
        + (2.0 * RATIO / 3.0) * cross
        + shear
        + (2.0 / 3.0) * twist
        + ((RATIO + 4.0) / 9.0) * cubic
    )


def kernel(
    ratio_in, density, void, fixed, disp, out,
    moved, fix, col_s, col_r, cor_s, cor_r, dens, dead, scale, energy, other, sens, mine, peer, hold, ratio,
    border, rim, held, local, send, recv, ready,
):
    layers, rows, depth = density.shape
    half = layers // 2
    r, c, h = lax.axis_index("gz"), lax.axis_index("gy"), 1 - lax.axis_index("lc")
    nr, nc = lax.axis_size("gz"), lax.axis_size("gy")
    dz = 1 - 2 * h
    mid = pl.ds(8, rows)
    low, high = pl.ds(0, 8), pl.ds(rows + 8, 8)

    def there(step_z, step_y):
        z, y = r + step_z, c + step_y
        return (z >= 0) & (z < nr) & (y >= 0) & (y < nc)

    def remote(index, src, dst, step_z, step_y, core, slot=None):
        copy = pltpu.make_async_remote_copy(
            src_ref=src, dst_ref=dst, send_sem=send.at[index if slot is None else slot],
            recv_sem=recv.at[index],
            device_id={"gz": r + step_z, "gy": c + step_y, "lc": 1 - core}, device_id_type=MESH,
        )
        goes, comes = there(step_z, step_y), there(-step_z, -step_y)
        return copy, goes, comes

    def between(index, src, dst, giver, slot=None):
        taker = 1 - giver
        copy, goes, comes = remote(index, src, dst, 0, 0, taker, slot)
        return copy, goes & (h == giver), comes & (h == taker)

    def flipped(index, src, dst, step_y, slot=None):
        copy, goes, _ = remote(index, src, dst, -dz, step_y, 1 - h, slot)
        return copy, goes, there(-dz, -step_y)

    def start(entry, when=True):
        copy, goes, _ = entry
        pl.when(goes & when)(copy.start)

    def arrive(entry):
        copy, _, comes = entry
        pl.when(comes)(copy.wait_recv)

    def left(entry):
        copy, goes, _ = entry
        pl.when(goes)(copy.wait_send)

    l0, b0 = half // 2 * (1 - h), half // 2 * h
    keep = half + 2
    lz, sb = (half + 2) * h, (layers - 2) * (1 - h)
    plane = pl.ds(0, rows)
    given, halo = (layers - 1) * (1 - h), (layers + 1) * h
    get_disp = pltpu.make_async_copy(
        disp.at[0], moved.at[:, pl.ds(1, layers), plane, :], local.at[0]
    )
    get_fix = pltpu.make_async_copy(fixed, fix, local.at[1])
    get_rim = pltpu.make_async_copy(disp.at[0, :, :, pl.ds(0, 1), :], rim, local.at[6])
    get_held = pltpu.make_async_copy(fixed.at[:, pl.ds(0, 1), :], held, local.at[7])
    get_dens = pltpu.make_async_copy(
        density.at[pl.ds(b0, keep)], dens.at[pl.ds(l0, keep), mid, :], local.at[2]
    )
    get_dead = pltpu.make_async_copy(void.at[pl.ds(half * h, half)], dead, local.at[3])
    get_ratio = pltpu.make_async_copy(ratio_in, ratio, local.at[4])
    get_border = pltpu.make_async_copy(density.at[pl.ds(sb, 2)], border, local.at[5])
    for copy in (get_rim, get_held, get_border, get_dens, get_disp, get_fix, get_ratio, get_dead):
        copy.start()

    barrier = pltpu.get_barrier_semaphore()
    def greet(semaphore, step_z, step_y, core):
        @pl.when(there(step_z, step_y))
        def _():
            pl.semaphore_signal(
                semaphore, inc=1,
                device_id={"gz": r + step_z, "gy": c + step_y, "lc": 1 - core},
                device_id_type=MESH,
            )

    flag = lambda value: value.astype(jnp.int32)

    def await_from(semaphore, step_z, step_y, count):
        @pl.when(there(step_z, step_y))
        def _():
            pl.semaphore_wait(semaphore, count)

    for core in (h, 1 - h):
        greet(barrier, 1, 0, core)
        greet(barrier, 0, 1, core)

    @pl.when(h == 1)
    def _():
        greet(barrier, 0, 0, 0)

    near, far = pl.ds(l0, keep), pl.ds(lz, 2)
    zs, zd = pl.ds(2 + (half - 2) * h, 2), pl.ds((half + 2) * (1 - h), 2)
    tiles = rows // SHORT
    head = (tiles - 2) * SHORT
    swap_rows = [pl.ds(0, head), pl.ds(head, rows - head)]
    top, bottom = pl.ds(rows - EDGE, EDGE), pl.ds(0, EDGE)
    above, below = pl.ds(8 - EDGE, EDGE), pl.ds(rows + 8, EDGE)
    last, first = pl.ds(rows + 8 - EDGE, EDGE), pl.ds(8, EDGE)
    dens_rows = [
        remote(1, dens.at[near, last, :], dens.at[near, above, :], 0, 1, h),
        remote(2, dens.at[near, first, :], dens.at[near, below, :], 0, -1, h),
    ]
    dens_far = [
        remote(0, border, dens.at[far, mid, :], dz, 0, h),
        flipped(3, dens.at[zs, last, :], dens.at[zd, above, :], 1),
        flipped(4, dens.at[zs, first, :], dens.at[zd, below, :], -1),
    ]

    def free_layer(i):
        free = (1 - fix[i]).astype(jnp.float32)
        for comp in range(3):
            moved[comp, i + 1, plane, :] = moved[comp, i + 1, plane, :] * free

    tall = rows // CHUNKS
    parts = [pl.ds(0, tall + SHORT), pl.ds(tall + SHORT, rows - tall - SHORT)]
    halves = [pl.ds(q * tall, tall) for q in range(CHUNKS)]
    send_disp = [
        remote(5 + q, moved.at[:, given + 1, part, :], moved.at[:, halo, part, :], dz, 0, h)
        for q, part in enumerate(parts)
    ]
    send_col = remote(7, col_s, col_r, 0, -1, h)
    send_cor = remote(8, cor_s, cor_r, dz, -1, h)
    awaited = 2 * (flag(r > 0) + flag(c > 0)) + (1 - h)

    @pl.when(awaited > 0)
    def _():
        pl.semaphore_wait(barrier, awaited)

    for core in (h, 1 - h):
        greet(ready.at[0], -1, 0, core)
        greet(ready.at[1], 0, -1, core)

    @pl.when(h == 0)
    def _():
        greet(ready.at[4], 0, 0, 1)

    get_rim.wait()
    get_held.wait()
    for i in range(layers):
        free = (1 - held[i]).astype(jnp.float32)
        for comp in range(3):
            col_s[comp, i : i + 1, :] = rim[comp, i] * free
    start(send_col)
    for comp in range(3):
        cor_s[comp : comp + 1, :] = rim[comp, given] * (1 - held[given]).astype(jnp.float32)
    get_border.wait()
    start(dens_far[0], h == 1)
    get_dens.wait()
    start(dens_rows[1])
    get_disp.wait()
    await_from(ready.at[1], 0, 1, 2)
    greet(ready.at[2], 0, 1, h)
    start(dens_rows[0])
    start(dens_far[1], h == 0)
    await_from(ready.at[0], 1, 0, 2)
    greet(ready.at[3], 0, -1, h)
    start(dens_far[2], h == 1)
    start(dens_far[0], h == 0)
    start(send_cor, h == 0)
    get_fix.wait()

    def free_step(i, _):
        free_layer(i)
        return 0

    lax.fori_loop(0, layers, free_step, 0)
    start(send_disp[0])
    await_from(ready.at[2], 0, -1, 1)
    start(dens_far[2], h == 0)
    start(send_cor, h == 1)

    get_ratio.wait()
    ratio_sum = ratio[0]
    for case in range(1, ratio.shape[0]):
        ratio_sum = ratio_sum + ratio[case]
    total = jnp.full((8, depth), ratio_sum.astype(jnp.float32))
    share = (SHEAR / 16.0) * (jnp.full((8, depth), ratio[1 - h].astype(jnp.float32)) / total)


    def energy_rows(first, count, j):
        row = pl.multiple_of(j * SHORT, SHORT)
        lower = node_modes(moved, first + 1, row)
        for k in range(count):
            upper = node_modes(moved, first + k + 2, row)
            energy[first + k, pl.ds(row, SHORT), :] = share * energy_tile(lower, upper)
            lower = upper

    def energy_layers(first, count, begin, end):
        def tile(j, _):
            energy_rows(first, count, begin + 2 * j)
            energy_rows(first, count, begin + 2 * j + 1)
            return 0

        lax.fori_loop(0, (end - begin) // 2, tile, 0)

    close, wide = 2 * (1 - h), 2 * h

    def scale_rows(j, row):
        cones = cone_tiles(dens, j, row, 2)
        for n in range(2):
            weights = weight_tile(
                r * layers + half * h + j + n, nr * layers, c * rows + row, nc * rows, depth
            )
            inverse = 1.0 / weights
            physical = cones[n] * inverse
            alive = (1 - dead[j + n, pl.ds(row, TALL), :]).astype(jnp.float32)
            scale[j + n, pl.ds(row, TALL), :] = (
                alive * (-3.0 * (1.0 - 0.001)) * physical * physical * inverse
            )

    def scale_two(j):
        def tile(k, _):
            scale_rows(j, pl.multiple_of(k * TALL, TALL))
            return 0

        lax.fori_loop(0, rows // TALL, tile, 0)

    give = half * (1 - h)
    swap_a = [
        remote(
            9, energy.at[pl.ds(give, half - 1), part, :],
            other.at[pl.ds(0, half - 1), part, :], 0, 0, 1 - h,
        )
        for q, part in enumerate(swap_rows)
    ]
    swap_b = [
        between(10, energy.at[half - 1, part, :], other.at[half - 1, part, :], 1)
        for q, part in enumerate(swap_rows)
    ]
    swap_whole = [
        remote(9, energy.at[pl.ds(give, half - 1)], other.at[pl.ds(0, half - 1)], 0, 0, 1 - h),
        between(10, energy.at[half - 1], other.at[half - 1], 1),
    ]
    rest = (half - 1) * h
    energy_layers(give, half - 1, 0, tiles - 2)
    pl.when(h == 1)(lambda: pl.semaphore_wait(ready.at[4], 1))
    start(swap_a[0])
    energy_layers(rest, half, 0, tiles - 2)
    start(swap_b[0])
    await_from(ready.at[3], 0, 1, 1)
    start(dens_far[1], h == 1)
    start(send_disp[1])

    blank = jnp.zeros((8, depth), jnp.float32)

    @pl.when(r == nr - 1)
    def _():
        for comp in range(3):
            moved[comp, layers + 1, plane, :] = jnp.zeros((rows, depth), jnp.float32)
            moved[comp, layers + 1, pl.ds(rows, 8), :] = blank

    @pl.when(c == nc - 1)
    def _():
        col_r[...] = jnp.zeros_like(col_r)

    @pl.when(jnp.logical_not(there(-dz, 1)))
    def _():
        cor_r[...] = jnp.zeros_like(cor_r)

    @pl.when(c == 0)
    def _():
        mine[low, :] = blank
        peer[low, :] = blank

    @pl.when(c == nc - 1)
    def _():
        mine[high, :] = blank
        peer[high, :] = blank

    for ref in (dens, sens):

        @pl.when(c == 0)
        def _():
            for i in range(half + 4):
                ref[i, low, :] = blank

        @pl.when(c == nc - 1)
        def _():
            for i in range(half + 4):
                ref[i, high, :] = blank

        @pl.when(jnp.logical_not(there(-dz, 0)))
        def _():
            for i in range(2):
                ref[lz + i] = jnp.zeros((rows + 16, depth), jnp.float32)

    arrive(send_col)
    for comp in range(3):
        for i in range(layers):
            moved[comp, i + 1, pl.ds(rows, 1), :] = col_r[comp, i : i + 1, :]
    energy_layers(give, half - 1, tiles - 2, tiles)
    start(swap_a[1])
    energy_layers(rest, half, tiles - 2, tiles)
    start(swap_b[1])
    get_dead.wait()
    for entry in dens_rows:
        arrive(entry)
    scale_two(close)

    def sense(j):
        sens[2 + j, mid, :] = scale[j] * (energy[half * h + j] + other[j])

    strip_count = rows // TALL
    arrive(dens_far[0])
    for k in range(strip_count):
        strip = (k + strip_count - c % strip_count) % strip_count
        for entry, at in ((dens_far[1], 0), (dens_far[2], strip_count - 1)):
            copy, goes, comes = entry
            arrive((copy, goes, comes & (strip == at)))
        scale_rows(wide, pl.multiple_of(strip * TALL, TALL))
    arrive(swap_whole[0])

    ps, pd = pl.ds(half - (half - 2) * h, 2), pl.ds((half + 2) * h, 2)
    close_copies = [
        remote(11, sens.at[ps, mid, :], sens.at[pd, mid, :], 0, 0, 1 - h),
        remote(14, sens.at[ps, last, :], sens.at[pd, above, :], 0, 1, 1 - h),
        remote(15, sens.at[ps, first, :], sens.at[pd, below, :], 0, -1, 1 - h),
    ]
    low_half, high_half = pl.ds(8, tall), pl.ds(8 + tall, rows - tall)
    wide_copies = [
        flipped(16, sens.at[zs, last, :], sens.at[zd, above, :], 1),
        flipped(17, sens.at[zs, first, :], sens.at[zd, below, :], -1),
        flipped(18, sens.at[zs, low_half, :], sens.at[zd, low_half, :], 0),
        flipped(18, sens.at[zs, high_half, :], sens.at[zd, high_half, :], 0),
    ]
    wide_whole = [*wide_copies[:2], flipped(18, sens.at[zs, mid, :], sens.at[zd, mid, :], 0)]
    core_rows = pl.ds(2, half)
    row_copies = [
        remote(12, sens.at[core_rows, last, :], sens.at[core_rows, above, :], 0, 1, h),
        remote(13, sens.at[core_rows, first, :], sens.at[core_rows, below, :], 0, -1, h),
    ]
    edge_copies = [
        remote(19, mine.at[last, :], mine.at[above, :], 0, 1, h, 0),
        remote(20, mine.at[first, :], mine.at[below, :], 0, -1, h, 1),
        flipped(21, mine.at[last, :], peer.at[above, :], 1, 2),
        flipped(22, mine.at[first, :], peer.at[below, :], -1, 3),
    ]
    main_copies = [
        flipped(23, mine.at[pl.ds(8 + q * tall, tall), :], peer.at[pl.ds(8 + q * tall, tall), :], 0, 4)
        for q in range(CHUNKS)
    ]
    main_whole = flipped(23, mine.at[mid, :], peer.at[mid, :], 0, 4)
    atop = (r == nr - 1) & (h == 0)
    whole = energy.at[layers - 1]
    top_copies = [
        remote(21, whole.at[top, :], peer.at[above, :], 0, 1, 1, 6),
        remote(22, whole.at[bottom, :], peer.at[below, :], 0, -1, 1, 7),
        remote(23, whole.at[halves[0], :], peer.at[pl.ds(8, tall), :], 0, 0, 1, 8),
        remote(23, whole.at[halves[1], :], peer.at[pl.ds(8 + tall, tall), :], 0, 0, 1, 8),
    ]
    top_copies = [
        (copy, goes & atop, comes & (r == nr - 1) & (h == 1)) for copy, goes, comes in top_copies
    ]
    top_whole, _, _ = remote(23, whole.at[plane, :], peer.at[mid, :], 0, 0, 1, 8)
    top_whole = [*top_copies[:2], (top_whole, atop, False)]
    joined = (h == 1) | (r > 0)
    edge_copies[:2] = [(copy, goes & joined, comes & joined) for copy, goes, comes in edge_copies[:2]]
    arrivals = [
        (copy, goes, comes | extra)
        for (copy, goes, comes), (_, _, extra) in zip(edge_copies[2:] + [main_whole], top_copies)
    ]
    pieces = [
        [edge_copies[1], edge_copies[3], main_copies[0]],
        [edge_copies[0], edge_copies[2], main_copies[1]],
    ]

    def boundary():
        for entry in [*dens_rows, *dens_far, *send_disp, send_col, send_cor, *swap_whole]:
            left(entry)

        arrive(send_cor)
        for comp in range(3):
            moved[comp, halo, pl.ds(rows, 1), :] = cor_r[comp : comp + 1, :]
        for q in range(CHUNKS):
            arrive(send_disp[q])

            @pl.when(joined)
            def _():
                for n in range(tall // SHORT):
                    row = q * tall + n * SHORT
                    mine[pl.ds(row + 8, SHORT), :] = share * energy_tile(
                        node_modes(moved, layers * h, row), node_modes(moved, layers * h + 1, row)
                    )

            for entry in pieces[q]:
                start(entry)
            if q == 0:
                start(wide_copies[3], c > 0)

        @pl.when(atop)
        def _():
            energy_layers(layers - 1, 1, 0, tiles)

        for entry in top_copies:
            start(entry)

    def spread():
        sense(wide)

        @pl.when(h == 0)
        def _():
            sense(1)

        @pl.when(h == 1)
        def _():
            sens[half + 1, mid, :] = scale[half - 1]

        for entry in wide_copies[:3]:
            start(entry)
        start(wide_copies[3], c == 0)
        arrive(swap_whole[1])
        sense(close)
        sense(close + 1)
        for entry in close_copies + row_copies:
            start(entry)

    spread()
    boundary()

    def filter_rows(j, count, row):
        cones = cone_tiles(sens, j, row, count)
        for n in range(count):
            alive = (1 - dead[j + n, pl.ds(row, TALL), :]).astype(jnp.float32)
            out[half * h + j + n, pl.ds(row, TALL), :] = alive * cones[n]

    def filter_layers(j, count):
        def tile(k, _):
            filter_rows(j, count, pl.multiple_of(k * TALL, TALL))
            return 0

        lax.fori_loop(0, rows // TALL, tile, 0)

    def partial_layers(j, count):
        def tile(k, _):
            row = pl.multiple_of(k * TALL, TALL)
            for n, cone in enumerate(cone_tiles(sens, j, row, count)):
                out[half * h + j + n, pl.ds(row, TALL), :] = cone
            return 0

        lax.fori_loop(0, rows // TALL, tile, 0)

    def hand_over(index, giver, j, count, part):
        place = out.at[pl.ds(half * giver + j, count), part, :]
        return between(index, place, place, giver, index - 15)

    early = [hand_over(24, 0, 2, half - 2, plane), hand_over(24, 1, 0, half - 3, plane)]
    strips = [pl.ds(k * TALL, TALL) for k in range(rows // TALL)]
    late = [
        [hand_over(25, 0, 0, 2, strip), hand_over(25, 1, half - 3, 3, strip)]
        for k, strip in enumerate(strips)
    ]
    for entry in close_copies + row_copies:
        arrive(entry)

    @pl.when(h == 0)
    def _():
        filter_layers(2, half - 2)

    @pl.when(h == 1)
    def _():
        filter_layers(0, half - 3)

    for entry in early:
        start(entry)
    for entry in close_copies + row_copies + wide_whole:
        left(entry)
    b = 1 + half * h

    def set_aside():
        hold[...] = sens[b]
        sens[b] = jnp.zeros((rows + 16, depth), jnp.float32)

    @pl.when(h == 1)
    def _():
        set_aside()
        partial_layers(half - 3, 1)

    for entry in wide_whole:
        arrive(entry)
    for entry in edge_copies + [main_whole] + top_whole:
        left(entry)
    pl.when((h == 0) & joined)(set_aside)

    @pl.when(h == 0)
    def _():
        partial_layers(0, 2)

    @pl.when(h == 1)
    def _():
        partial_layers(half - 2, 2)

    def finish_rows(pairs, row):
        for (j, reach), cone in zip(pairs, boundary_cones(sens, b, row, [p[1] for p in pairs])):
            alive = (1 - dead[j, pl.ds(row, TALL), :]).astype(jnp.float32)
            here = pl.ds(row, TALL)
            out[half * h + j, here, :] = alive * (out[half * h + j, here, :] + cone)

    for entry in edge_copies[:2] + arrivals:
        arrive(entry)

    @pl.when(joined)
    def _():
        sens[b] = hold[...] * (mine[...] + peer[...])

    for k in range(rows // TALL):

        @pl.when(h == 0)
        def _():
            finish_rows([(0, 1), (1, 2)], k * TALL)

        @pl.when(h == 1)
        def _():
            finish_rows([(half - 3, 2), (half - 2, 1), (half - 1, 0)], k * TALL)

        for entry in late[k]:
            start(entry)
    late = [hand_over(25, 0, 0, 2, plane), hand_over(25, 1, half - 3, 3, plane)]
    for entry in early + late:
        left(entry)
    for entry in early + late:
        arrive(entry)


def shards(density, void_mask, fixed_mask, displacement, load_ratio):
    layers, rows, depth = density.shape
    half = layers // 2
    f32 = jnp.float32
    hbm = pl.BlockSpec(memory_space=pl.ANY)
    return pl.pallas_call(
        kernel,
        out_shape=pltpu.VMEM(density.shape, f32),
        in_specs=[hbm] * 5,
        out_specs=pl.BlockSpec(memory_space=pltpu.VMEM),
        scratch_shapes=[
            pltpu.VMEM((3, layers + 2, rows + 8, depth), f32),
            pltpu.VMEM((layers, rows, depth), jnp.int32),
            pltpu.VMEM((3, layers, depth), f32),
            pltpu.VMEM((3, layers, depth), f32),
            pltpu.VMEM((8, depth), f32),
            pltpu.VMEM((8, depth), f32),
            pltpu.VMEM((half + 4, rows + 16, depth), f32),
            pltpu.VMEM((half, rows, depth), jnp.int32),
            pltpu.VMEM((half, rows, depth), f32),
            pltpu.VMEM((layers, rows, depth), f32),
            pltpu.VMEM((half, rows, depth), f32),
            pltpu.VMEM((half + 4, rows + 16, depth), f32),
            pltpu.VMEM((rows + 16, depth), f32),
            pltpu.VMEM((rows + 16, depth), f32),
            pltpu.VMEM((rows + 16, depth), f32),
            pltpu.SMEM(load_ratio.shape, load_ratio.dtype),
            pltpu.VMEM((2, rows, depth), f32),
            pltpu.VMEM((3, layers, 1, depth), f32),
            pltpu.VMEM((layers, 1, depth), jnp.int32),
            pltpu.SemaphoreType.DMA((8,)),
            pltpu.SemaphoreType.DMA((N_SEND,)),
            pltpu.SemaphoreType.DMA((N_RECV,)),
            pltpu.SemaphoreType.REGULAR((5,)),
        ],
        compiler_params=pltpu.CompilerParams(collective_id=0, has_side_effects=True),
    )(load_ratio, density, void_mask, fixed_mask, displacement)


def solution(mesh):
    placed = (
        P(("parts", "gz"), "gy", None),
        P(("parts", "gz"), "gy", None),
        P(("parts", "gz"), "gy", None),
        P("lc", None, ("parts", "gz"), "gy", None),
        P("parts"),
    )
    return jax.shard_map(
        shards,
        mesh=mesh,
        in_specs=placed,
        out_specs=P(("parts", "gz"), "gy", None),
        check_vma=False,
    )
```

```python
import math

import jax
import jax.numpy as jnp
from jax import lax
from jax.experimental import pallas as pl
from jax.experimental.pallas import tpu as pltpu
from jax.sharding import PartitionSpec as P

MESH = pl.DeviceIdType.MESH
POISSON = 0.3
FACTOR = 1.0 / ((1.0 + POISSON) * (1.0 - 2.0 * POISSON))
LAMBDA = POISSON * FACTOR
SHEAR = (0.5 - POISSON) * FACTOR
RATIO = LAMBDA / SHEAR
W = [2.5 - math.sqrt(d) for d in range(7)]
CHUNKS = 2
EDGE = 2
UNROLL = 6
N_SEND = 19
N_RECV = 26
TALL = 32
SHORT = 8


def layer_classes(q0, q1, q2, q4, q5):
    p0 = W[0] * q0 + W[1] * q1 + W[2] * q2 + W[4] * q4 + W[5] * q5
    p1 = W[1] * q0 + W[2] * q1 + W[3] * q2 + W[5] * q4 + W[6] * q5
    p2 = W[4] * q0 + W[5] * q1 + W[6] * q2
    return p0, p1, p2


def lane_index(shape):
    return lax.broadcasted_iota(jnp.int32, shape, len(shape) - 1)


def lane_pair(field, step):
    depth = field.shape[-1]
    lane = lane_index(field.shape)
    after = jnp.where(lane < depth - step, pltpu.roll(field, depth - step, 1), 0.0)
    before = jnp.where(lane >= step, pltpu.roll(field, step, 1), 0.0)
    return after + before


def cone_tiles(ref, layer, row, count):
    window = TALL + 16
    f = [ref[layer + k, pl.ds(row, window), :] for k in range(count + 4)]
    mid = slice(8, 8 + TALL)

    def pair(t, step):
        return (pltpu.roll(t, step, 0) + pltpu.roll(t, window - step, 0))[mid]

    result = []
    for k in range(count):
        x0, x1, x2 = f[k + 2], f[k + 1] + f[k + 3], f[k] + f[k + 4]
        q0 = x0[mid]
        q1 = x1[mid] + pair(x0, 1)
        q2 = pair(x1, 1)
        q4 = x2[mid] + pair(x0, 2)
        q5 = pair(x2, 1) + pair(x1, 2)
        p0, p1, p2 = layer_classes(q0, q1, q2, q4, q5)
        result.append(p0 + lane_pair(p1, 1) + lane_pair(p2, 2))
    return result


def boundary_cones(ref, layer, row, reaches):
    window = TALL + 16
    t = ref[layer, pl.ds(row, window), :]
    mid = slice(8, 8 + TALL)
    t0 = t[mid]
    t1, t2 = [
        (pltpu.roll(t, step, 0) + pltpu.roll(t, window - step, 0))[mid] for step in (1, 2)
    ]
    result = []
    for reach in reaches:
        if reach == 0:
            p0 = W[0] * t0 + W[1] * t1 + W[4] * t2
            p1 = W[1] * t0 + W[2] * t1 + W[5] * t2
            p2 = W[4] * t0 + W[5] * t1
        elif reach == 1:
            p0 = W[1] * t0 + W[2] * t1 + W[5] * t2
            p1 = W[2] * t0 + W[3] * t1 + W[6] * t2
            p2 = W[5] * t0 + W[6] * t1
        else:
            p0, p1, p2 = W[4] * t0 + W[5] * t1, W[5] * t0 + W[6] * t1, None
        total = p0 + lane_pair(p1, 1)
        result.append(total if p2 is None else total + lane_pair(p2, 2))
    return result


def present(position, total, step):
    before = (position >= step).astype(jnp.float32)
    return before + (position + step < total).astype(jnp.float32)


def weight_tile(layer, layers, row, rows, depth):
    shape = (TALL, depth)
    sub = lax.broadcasted_iota(jnp.int32, shape, 0) + row
    spot = jnp.full(shape, layer, jnp.int32)
    nx1, nx2 = present(spot, layers, 1), present(spot, layers, 2)
    ny1, ny2 = present(sub, rows, 1), present(sub, rows, 2)
    one = jnp.ones(shape, jnp.float32)
    p0, p1, p2 = layer_classes(one, nx1 + ny1, nx1 * ny1, nx2 + ny2, nx2 * ny1 + nx1 * ny2)
    lane = lane_index(shape)
    return p0 + present(lane, depth, 1) * p1 + present(lane, depth, 2) * p2


def node_modes(ref, layer, row):
    result = []
    for comp in range(3):
        t = ref[comp, layer, pl.ds(row, SHORT + 8), :]
        depth, window = t.shape[-1], t.shape[0]
        here, after = t[0:SHORT], pltpu.roll(t, window - 1, 0)[0:SHORT]
        s, d = here + after, after - here
        inner = lane_index(s.shape) < depth - 1
        sn = jnp.where(inner, pltpu.roll(s, depth - 1, 1), 0.0)
        dn = jnp.where(inner, pltpu.roll(d, depth - 1, 1), 0.0)
        result.append((s + sn, sn - s, d + dn, dn - d))
    return result


def energy_tile(lower, upper):
    modes = []
    for a, b in zip(lower, upper):
        modes.append(
            {
                "x": b[0] - a[0],
                "z": a[1] + b[1],
                "y": a[2] + b[2],
                "yz": a[3] + b[3],
                "xz": b[1] - a[1],
                "xy": b[2] - a[2],
                "xyz": b[3] - a[3],
            }
        )
    u, v, w = modes
    sq = lambda t: t * t
    trace = sq(u["x"] + v["y"] + w["z"])
    normal = sq(u["x"]) + sq(v["y"]) + sq(w["z"])
    bend = sq(u["xy"]) + sq(u["xz"]) + sq(v["xy"]) + sq(v["yz"]) + sq(w["yz"]) + sq(w["xz"])
    cross = v["xy"] * w["xz"] + u["xy"] * w["yz"] + u["xz"] * v["yz"]
    shear = sq(u["y"] + v["x"]) + sq(u["z"] + w["x"]) + sq(v["z"] + w["y"])
    pair = v["xz"] + w["xy"]
    twist = u["yz"] * (u["yz"] + pair) + v["xz"] * pair + sq(w["xy"])
    cubic = sq(u["xyz"]) + sq(v["xyz"]) + sq(w["xyz"])
    return (
        RATIO * trace
        + 2.0 * normal
        + (1.0 + RATIO / 3.0) * bend
        + (2.0 * RATIO / 3.0) * cross
        + shear
        + (2.0 / 3.0) * twist
        + ((RATIO + 4.0) / 9.0) * cubic
    )


def kernel(
    ratio_in, density, void, fixed, disp, out,
    moved, fix, col_s, col_r, cor_s, cor_r, dens, dead, scale, energy, other, sens, mine, peer, hold, ratio,
    border, rim, held, local, send, recv, ready,
):
    layers, rows, depth = density.shape
    half = layers // 2
    r, c, h = lax.axis_index("gz"), lax.axis_index("gy"), 1 - lax.axis_index("lc")
    nr, nc = lax.axis_size("gz"), lax.axis_size("gy")
    dz = 1 - 2 * h
    mid = pl.ds(8, rows)
    low, high = pl.ds(0, 8), pl.ds(rows + 8, 8)

    def there(step_z, step_y):
        z, y = r + step_z, c + step_y
        return (z >= 0) & (z < nr) & (y >= 0) & (y < nc)

    def remote(index, src, dst, step_z, step_y, core, slot=None):
        copy = pltpu.make_async_remote_copy(
            src_ref=src, dst_ref=dst, send_sem=send.at[index if slot is None else slot],
            recv_sem=recv.at[index],
            device_id={"gz": r + step_z, "gy": c + step_y, "lc": 1 - core}, device_id_type=MESH,
        )
        goes, comes = there(step_z, step_y), there(-step_z, -step_y)
        return copy, goes, comes

    def between(index, src, dst, giver, slot=None):
        taker = 1 - giver
        copy, goes, comes = remote(index, src, dst, 0, 0, taker, slot)
        return copy, goes & (h == giver), comes & (h == taker)

    def flipped(index, src, dst, step_y, slot=None):
        copy, goes, _ = remote(index, src, dst, -dz, step_y, 1 - h, slot)
        return copy, goes, there(-dz, -step_y)

    def start(entry, when=True):
        copy, goes, _ = entry
        pl.when(goes & when)(copy.start)

    def arrive(entry):
        copy, _, comes = entry
        pl.when(comes)(copy.wait_recv)

    def left(entry):
        copy, goes, _ = entry
        pl.when(goes)(copy.wait_send)

    l0, b0 = half // 2 * (1 - h), half // 2 * h
    keep = half + 2
    lz, sb = (half + 2) * h, (layers - 2) * (1 - h)
    plane = pl.ds(0, rows)
    given, halo = (layers - 1) * (1 - h), (layers + 1) * h
    get_disp = pltpu.make_async_copy(
        disp.at[0], moved.at[:, pl.ds(1, layers), plane, :], local.at[0]
    )
    get_fix = pltpu.make_async_copy(fixed, fix, local.at[1])
    get_rim = pltpu.make_async_copy(disp.at[0, :, :, pl.ds(0, 1), :], rim, local.at[6])
    get_held = pltpu.make_async_copy(fixed.at[:, pl.ds(0, 1), :], held, local.at[7])
    get_dens = pltpu.make_async_copy(
        density.at[pl.ds(b0, keep)], dens.at[pl.ds(l0, keep), mid, :], local.at[2]
    )
    get_dead = pltpu.make_async_copy(void.at[pl.ds(half * h, half)], dead, local.at[3])
    get_ratio = pltpu.make_async_copy(ratio_in, ratio, local.at[4])
    get_border = pltpu.make_async_copy(density.at[pl.ds(sb, 2)], border, local.at[5])
    for copy in (get_rim, get_held, get_border, get_dens, get_disp, get_fix, get_ratio, get_dead):
        copy.start()

    barrier = pltpu.get_barrier_semaphore()
    def greet(semaphore, step_z, step_y, core):
        @pl.when(there(step_z, step_y))
        def _():
            pl.semaphore_signal(
                semaphore, inc=1,
                device_id={"gz": r + step_z, "gy": c + step_y, "lc": 1 - core},
                device_id_type=MESH,
            )

    flag = lambda value: value.astype(jnp.int32)

    def await_from(semaphore, step_z, step_y, count):
        @pl.when(there(step_z, step_y))
        def _():
            pl.semaphore_wait(semaphore, count)

    for core in (h, 1 - h):
        greet(barrier, 1, 0, core)
        greet(barrier, 0, 1, core)

    @pl.when(h == 1)
    def _():
        greet(barrier, 0, 0, 0)

    near, far = pl.ds(l0, keep), pl.ds(lz, 2)
    zs, zd = pl.ds(2 + (half - 2) * h, 2), pl.ds((half + 2) * (1 - h), 2)
    tiles = rows // SHORT
    head = (tiles - 2) * SHORT
    swap_rows = [pl.ds(0, head), pl.ds(head, rows - head)]
    top, bottom = pl.ds(rows - EDGE, EDGE), pl.ds(0, EDGE)
    above, below = pl.ds(8 - EDGE, EDGE), pl.ds(rows + 8, EDGE)
    last, first = pl.ds(rows + 8 - EDGE, EDGE), pl.ds(8, EDGE)
    dens_rows = [
        remote(1, dens.at[near, last, :], dens.at[near, above, :], 0, 1, h),
        remote(2, dens.at[near, first, :], dens.at[near, below, :], 0, -1, h),
    ]
    dens_far = [
        remote(0, border, dens.at[far, mid, :], dz, 0, h),
        flipped(3, dens.at[zs, last, :], dens.at[zd, above, :], 1),
        flipped(4, dens.at[zs, first, :], dens.at[zd, below, :], -1),
    ]

    def free_layer(i):
        free = (1 - fix[i]).astype(jnp.float32)
        for comp in range(3):
            moved[comp, i + 1, plane, :] = moved[comp, i + 1, plane, :] * free

    tall = rows // CHUNKS
    split = tall - SHORT
    spans = [(0, split), (split, rows - split)]
    parts = [pl.ds(0, split + SHORT), pl.ds(split + SHORT, rows - split - SHORT)]
    send_disp = [
        remote(5 + q, moved.at[:, given + 1, part, :], moved.at[:, halo, part, :], dz, 0, h)
        for q, part in enumerate(parts)
    ]
    send_col = remote(7, col_s, col_r, 0, -1, h)
    send_cor = remote(8, cor_s, cor_r, dz, -1, h)
    awaited = 2 * (flag(r > 0) + flag(c > 0)) + (1 - h)

    @pl.when(awaited > 0)
    def _():
        pl.semaphore_wait(barrier, awaited)

    for core in (h, 1 - h):
        greet(ready.at[0], -1, 0, core)
        greet(ready.at[1], 0, -1, core)

    @pl.when(h == 0)
    def _():
        greet(ready.at[4], 0, 0, 1)

    get_rim.wait()
    get_held.wait()
    for i in range(layers):
        free = (1 - held[i]).astype(jnp.float32)
        for comp in range(3):
            col_s[comp, i : i + 1, :] = rim[comp, i] * free
    start(send_col)
    for comp in range(3):
        cor_s[comp : comp + 1, :] = rim[comp, given] * (1 - held[given]).astype(jnp.float32)
    get_border.wait()
    start(dens_far[0], h == 1)
    get_dens.wait()
    start(dens_rows[1])
    get_disp.wait()
    await_from(ready.at[1], 0, 1, 2)
    greet(ready.at[2], 0, 1, h)
    start(dens_rows[0])
    start(dens_far[1], h == 0)
    await_from(ready.at[0], 1, 0, 2)
    greet(ready.at[3], 0, -1, h)
    start(dens_far[2], h == 1)
    start(dens_far[0], h == 0)
    start(send_cor, h == 0)
    get_fix.wait()

    def free_step(i, _):
        free_layer(i)
        return 0

    lax.fori_loop(0, layers, free_step, 0)
    start(send_disp[0])
    await_from(ready.at[2], 0, -1, 1)
    start(dens_far[2], h == 0)
    start(send_cor, h == 1)

    get_ratio.wait()
    ratio_sum = ratio[0]
    for case in range(1, ratio.shape[0]):
        ratio_sum = ratio_sum + ratio[case]
    total = jnp.full((8, depth), ratio_sum.astype(jnp.float32))
    share = (SHEAR / 16.0) * (jnp.full((8, depth), ratio[1 - h].astype(jnp.float32)) / total)


    def energy_rows(first, count, j):
        row = pl.multiple_of(j * SHORT, SHORT)
        lower = node_modes(moved, first + 1, row)
        for k in range(count):
            upper = node_modes(moved, first + k + 2, row)
            energy[first + k, pl.ds(row, SHORT), :] = share * energy_tile(lower, upper)
            lower = upper

    def energy_layers(first, count, begin, end):
        step = math.gcd(end - begin, UNROLL)

        def tile(j, _):
            for n in range(step):
                energy_rows(first, count, begin + step * j + n)
            return 0

        lax.fori_loop(0, (end - begin) // step, tile, 0)

    close, wide = 2 * (1 - h), 2 * h

    def scale_rows(j, row):
        cones = cone_tiles(dens, j, row, 2)
        for n in range(2):
            weights = weight_tile(
                r * layers + half * h + j + n, nr * layers, c * rows + row, nc * rows, depth
            )
            inverse = 1.0 / weights
            physical = cones[n] * inverse
            alive = (1 - dead[j + n, pl.ds(row, TALL), :]).astype(jnp.float32)
            scale[j + n, pl.ds(row, TALL), :] = (
                alive * (-3.0 * (1.0 - 0.001)) * physical * physical * inverse
            )

    def scale_two(j):
        def tile(k, _):
            scale_rows(j, pl.multiple_of(k * TALL, TALL))
            return 0

        lax.fori_loop(0, rows // TALL, tile, 0)

    give = half * (1 - h)
    swap_a = [
        remote(
            9, energy.at[pl.ds(give, half - 1), part, :],
            other.at[pl.ds(0, half - 1), part, :], 0, 0, 1 - h,
        )
        for q, part in enumerate(swap_rows)
    ]
    swap_b = [
        between(10, energy.at[half - 1, part, :], other.at[half - 1, part, :], 1)
        for q, part in enumerate(swap_rows)
    ]
    swap_whole = [
        remote(9, energy.at[pl.ds(give, half - 1)], other.at[pl.ds(0, half - 1)], 0, 0, 1 - h),
        between(10, energy.at[half - 1], other.at[half - 1], 1),
    ]
    rest = (half - 1) * h
    energy_layers(give, half - 1, 0, tiles - 2)
    pl.when(h == 1)(lambda: pl.semaphore_wait(ready.at[4], 1))
    start(swap_a[0])
    energy_layers(rest, half, 0, tiles - 2)
    start(swap_b[0])
    await_from(ready.at[3], 0, 1, 1)
    start(dens_far[1], h == 1)
    start(send_disp[1])

    blank = jnp.zeros((8, depth), jnp.float32)

    @pl.when(r == nr - 1)
    def _():
        for comp in range(3):
            moved[comp, layers + 1, plane, :] = jnp.zeros((rows, depth), jnp.float32)
            moved[comp, layers + 1, pl.ds(rows, 8), :] = blank

    @pl.when(c == nc - 1)
    def _():
        col_r[...] = jnp.zeros_like(col_r)

    @pl.when(jnp.logical_not(there(-dz, 1)))
    def _():
        cor_r[...] = jnp.zeros_like(cor_r)

    @pl.when(c == 0)
    def _():
        mine[low, :] = blank
        peer[low, :] = blank

    @pl.when(c == nc - 1)
    def _():
        mine[high, :] = blank
        peer[high, :] = blank

    for ref in (dens, sens):

        @pl.when(c == 0)
        def _():
            for i in range(half + 4):
                ref[i, low, :] = blank

        @pl.when(c == nc - 1)
        def _():
            for i in range(half + 4):
                ref[i, high, :] = blank

        @pl.when(jnp.logical_not(there(-dz, 0)))
        def _():
            for i in range(2):
                ref[lz + i] = jnp.zeros((rows + 16, depth), jnp.float32)

    arrive(send_col)
    for comp in range(3):
        for i in range(layers):
            moved[comp, i + 1, pl.ds(rows, 1), :] = col_r[comp, i : i + 1, :]
    energy_layers(give, half - 1, tiles - 2, tiles)
    start(swap_a[1])
    energy_layers(rest, half, tiles - 2, tiles)
    start(swap_b[1])
    get_dead.wait()
    for entry in dens_rows:
        arrive(entry)
    scale_two(close)

    def sense(j):
        sens[2 + j, mid, :] = scale[j] * (energy[half * h + j] + other[j])

    strip_count = rows // TALL
    arrive(dens_far[0])
    for k in range(strip_count):
        strip = (k + strip_count - c % strip_count) % strip_count
        for entry, at in ((dens_far[1], 0), (dens_far[2], strip_count - 1)):
            copy, goes, comes = entry
            arrive((copy, goes, comes & (strip == at)))
        scale_rows(wide, pl.multiple_of(strip * TALL, TALL))
    arrive(swap_whole[0])

    ps, pd = pl.ds(half - (half - 2) * h, 2), pl.ds((half + 2) * h, 2)
    close_copies = [
        remote(11, sens.at[ps, mid, :], sens.at[pd, mid, :], 0, 0, 1 - h),
        remote(14, sens.at[ps, last, :], sens.at[pd, above, :], 0, 1, 1 - h),
        remote(15, sens.at[ps, first, :], sens.at[pd, below, :], 0, -1, 1 - h),
    ]
    low_half, high_half = pl.ds(8, tall), pl.ds(8 + tall, rows - tall)
    wide_copies = [
        flipped(16, sens.at[zs, last, :], sens.at[zd, above, :], 1),
        flipped(17, sens.at[zs, first, :], sens.at[zd, below, :], -1),
        flipped(18, sens.at[zs, low_half, :], sens.at[zd, low_half, :], 0),
        flipped(18, sens.at[zs, high_half, :], sens.at[zd, high_half, :], 0),
    ]
    wide_whole = [*wide_copies[:2], flipped(18, sens.at[zs, mid, :], sens.at[zd, mid, :], 0)]
    core_rows = pl.ds(2, half)
    row_copies = [
        remote(12, sens.at[core_rows, last, :], sens.at[core_rows, above, :], 0, 1, h),
        remote(13, sens.at[core_rows, first, :], sens.at[core_rows, below, :], 0, -1, h),
    ]
    edge_copies = [
        remote(19, mine.at[last, :], mine.at[above, :], 0, 1, h, 0),
        remote(20, mine.at[first, :], mine.at[below, :], 0, -1, h, 1),
        flipped(21, mine.at[last, :], peer.at[above, :], 1, 2),
        flipped(22, mine.at[first, :], peer.at[below, :], -1, 3),
    ]
    main_copies = [
        flipped(23, mine.at[pl.ds(8 + begin, size), :], peer.at[pl.ds(8 + begin, size), :], 0, 4)
        for begin, size in spans
    ]
    main_whole = flipped(23, mine.at[mid, :], peer.at[mid, :], 0, 4)
    atop = (r == nr - 1) & (h == 0)
    whole = energy.at[layers - 1]
    top_copies = [
        remote(21, whole.at[top, :], peer.at[above, :], 0, 1, 1, 6),
        remote(22, whole.at[bottom, :], peer.at[below, :], 0, -1, 1, 7),
        remote(23, whole.at[pl.ds(0, split), :], peer.at[pl.ds(8, split), :], 0, 0, 1, 8),
        remote(23, whole.at[pl.ds(split, rows - split), :], peer.at[pl.ds(8 + split, rows - split), :], 0, 0, 1, 8),
    ]
    top_copies = [
        (copy, goes & atop, comes & (r == nr - 1) & (h == 1)) for copy, goes, comes in top_copies
    ]
    top_whole, _, _ = remote(23, whole.at[plane, :], peer.at[mid, :], 0, 0, 1, 8)
    top_whole = [*top_copies[:2], (top_whole, atop, False)]
    joined = (h == 1) | (r > 0)
    edge_copies[:2] = [(copy, goes & joined, comes & joined) for copy, goes, comes in edge_copies[:2]]
    arrivals = [
        (copy, goes, comes | extra)
        for (copy, goes, comes), (_, _, extra) in zip(edge_copies[2:] + [main_whole], top_copies)
    ]
    pieces = [
        [edge_copies[1], edge_copies[3], main_copies[0]],
        [edge_copies[0], edge_copies[2], main_copies[1]],
    ]

    def boundary():
        for entry in [*dens_rows, *dens_far, *send_disp, send_col, send_cor, *swap_whole]:
            left(entry)

        arrive(send_cor)
        for comp in range(3):
            moved[comp, halo, pl.ds(rows, 1), :] = cor_r[comp : comp + 1, :]
        for q in range(CHUNKS):
            arrive(send_disp[q])

            @pl.when(joined)
            def _():
                begin, size = spans[q]
                for row in range(begin, begin + size, SHORT):
                    mine[pl.ds(row + 8, SHORT), :] = share * energy_tile(
                        node_modes(moved, layers * h, row), node_modes(moved, layers * h + 1, row)
                    )

            for entry in pieces[q]:
                start(entry)
            if q == 0:
                start(wide_copies[3], c > 0)

        @pl.when(atop)
        def _():
            energy_layers(layers - 1, 1, 0, tiles)

        for entry in top_copies:
            start(entry)

    def spread():
        sense(wide)

        @pl.when(h == 0)
        def _():
            sense(1)

        @pl.when(h == 1)
        def _():
            sens[half + 1, mid, :] = scale[half - 1]

        for entry in wide_copies[:3]:
            start(entry)
        start(wide_copies[3], c == 0)
        arrive(swap_whole[1])
        sense(close)
        sense(close + 1)
        for entry in close_copies + row_copies:
            start(entry)

    spread()
    boundary()

    def filter_rows(j, count, row):
        cones = cone_tiles(sens, j, row, count)
        for n in range(count):
            alive = (1 - dead[j + n, pl.ds(row, TALL), :]).astype(jnp.float32)
            out[half * h + j + n, pl.ds(row, TALL), :] = alive * cones[n]

    def filter_layers(j, count):
        def tile(k, _):
            filter_rows(j, count, pl.multiple_of(k * TALL, TALL))
            return 0

        lax.fori_loop(0, rows // TALL, tile, 0)

    def partial_rows(j, count, row):
        for n, cone in enumerate(cone_tiles(sens, j, row, count)):
            out[half * h + j + n, pl.ds(row, TALL), :] = cone

    def partial_layers(j, count):
        def tile(k, _):
            partial_rows(j, count, pl.multiple_of(k * TALL, TALL))
            return 0

        lax.fori_loop(0, rows // TALL, tile, 0)

    def hand_over(index, giver, j, count, part):
        place = out.at[pl.ds(half * giver + j, count), part, :]
        return between(index, place, place, giver, index - 15)

    early = [hand_over(24, 0, 2, half - 2, plane), hand_over(24, 1, 0, half - 3, plane)]
    strips = [pl.ds(k * TALL, TALL) for k in range(rows // TALL)]
    late = [
        [hand_over(25, 0, 0, 2, strip), hand_over(25, 1, half - 3, 3, strip)]
        for k, strip in enumerate(strips)
    ]
    for entry in [*close_copies[:2], row_copies[0]]:
        arrive(entry)
    for entry in close_copies + row_copies + wide_whole:
        left(entry)
    b = 1 + half * h

    def set_aside(part):
        hold[part, :] = sens[b, part, :]
        sens[b, part, :] = jnp.zeros((part.size, depth), jnp.float32)

    upper, rim_rows = pl.ds(0, rows + 8), pl.ds(rows + 8, 8)
    pl.when(h == 1)(lambda: set_aside(upper))

    def early_rows(row):
        @pl.when(h == 0)
        def _():
            filter_rows(2, half - 2, row)

        @pl.when(h == 1)
        def _():
            filter_rows(0, half - 3, row)
            partial_rows(half - 3, 1, row)

    for k in range(rows // TALL - 1):
        early_rows(k * TALL)
    for entry in [close_copies[2], row_copies[1]]:
        arrive(entry)
    pl.when(h == 1)(lambda: set_aside(rim_rows))
    early_rows(rows - TALL)
    for entry in early:
        start(entry)
    for entry in wide_whole:
        arrive(entry)
    for entry in edge_copies + [main_whole] + top_whole:
        left(entry)
    @pl.when((h == 0) & joined)
    def _():
        set_aside(upper)
        set_aside(rim_rows)

    @pl.when(h == 0)
    def _():
        partial_layers(0, 2)

    @pl.when(h == 1)
    def _():
        partial_layers(half - 2, 2)

    def finish_rows(pairs, row):
        for (j, reach), cone in zip(pairs, boundary_cones(sens, b, row, [p[1] for p in pairs])):
            alive = (1 - dead[j, pl.ds(row, TALL), :]).astype(jnp.float32)
            here = pl.ds(row, TALL)
            out[half * h + j, here, :] = alive * (out[half * h + j, here, :] + cone)

    for entry in edge_copies[:2] + arrivals:
        arrive(entry)

    @pl.when(joined)
    def _():
        sens[b] = hold[...] * (mine[...] + peer[...])

    for k in range(rows // TALL):

        @pl.when(h == 0)
        def _():
            finish_rows([(0, 1), (1, 2)], k * TALL)

        @pl.when(h == 1)
        def _():
            finish_rows([(half - 3, 2), (half - 2, 1), (half - 1, 0)], k * TALL)

        for entry in late[k]:
            start(entry)
    late = [hand_over(25, 0, 0, 2, plane), hand_over(25, 1, half - 3, 3, plane)]
    for entry in early + late:
        left(entry)
    for entry in early + late:
        arrive(entry)


def shards(density, void_mask, fixed_mask, displacement, load_ratio):
    layers, rows, depth = density.shape
    half = layers // 2
    f32 = jnp.float32
    hbm = pl.BlockSpec(memory_space=pl.ANY)
    return pl.pallas_call(
        kernel,
        out_shape=pltpu.VMEM(density.shape, f32),
        in_specs=[hbm] * 5,
        out_specs=pl.BlockSpec(memory_space=pltpu.VMEM),
        scratch_shapes=[
            pltpu.VMEM((3, layers + 2, rows + 8, depth), f32),
            pltpu.VMEM((layers, rows, depth), jnp.int32),
            pltpu.VMEM((3, layers, depth), f32),
            pltpu.VMEM((3, layers, depth), f32),
            pltpu.VMEM((8, depth), f32),
            pltpu.VMEM((8, depth), f32),
            pltpu.VMEM((half + 4, rows + 16, depth), f32),
            pltpu.VMEM((half, rows, depth), jnp.int32),
            pltpu.VMEM((half, rows, depth), f32),
            pltpu.VMEM((layers, rows, depth), f32),
            pltpu.VMEM((half, rows, depth), f32),
            pltpu.VMEM((half + 4, rows + 16, depth), f32),
            pltpu.VMEM((rows + 16, depth), f32),
            pltpu.VMEM((rows + 16, depth), f32),
            pltpu.VMEM((rows + 16, depth), f32),
            pltpu.SMEM(load_ratio.shape, load_ratio.dtype),
            pltpu.VMEM((2, rows, depth), f32),
            pltpu.VMEM((3, layers, 1, depth), f32),
            pltpu.VMEM((layers, 1, depth), jnp.int32),
            pltpu.SemaphoreType.DMA((8,)),
            pltpu.SemaphoreType.DMA((N_SEND,)),
            pltpu.SemaphoreType.DMA((N_RECV,)),
            pltpu.SemaphoreType.REGULAR((5,)),
        ],
        compiler_params=pltpu.CompilerParams(collective_id=0, has_side_effects=True),
    )(load_ratio, density, void_mask, fixed_mask, displacement)


def solution(mesh):
    placed = (
        P(("parts", "gz"), "gy", None),
        P(("parts", "gz"), "gy", None),
        P(("parts", "gz"), "gy", None),
        P("lc", None, ("parts", "gz"), "gy", None),
        P("parts"),
    )
    return jax.shard_map(
        shards,
        mesh=mesh,
        in_specs=placed,
        out_specs=P(("parts", "gz"), "gy", None),
        check_vma=False,
    )
```
